256 devices in a mesh: dp: 32 (over x, z), expert: 8 (over y, core).
Axes of the slice: x: 4, y: 4, z: 8, core: 2. Of those that a mesh axis runs over, the one named last changes fastest.
Arguments:
- tokens: bfloat16 [32768, 2048], P(('dp', 'expert')), may hold values from -6 to 6
- expert_ids: int32 [32768, 8], P(('dp', 'expert')), may hold values from 0 to 127, all different within a row
- route_probs: float32 [32768, 8], P(('dp', 'expert')), may hold values from 0.05 to 1
- shard_limit: int32 [256, 128], P(('dp', 'expert')), may hold values from 4 to 8
- gate_proj: bfloat16 [256, 2048, 384], P(('dp', 'expert')), may hold values from -0.125 to 0.125
- up_proj: bfloat16 [256, 2048, 384], P(('dp', 'expert')), may hold values from -0.125 to 0.125
- down_proj: bfloat16 [256, 384, 2048], P(('dp', 'expert')), may hold values from -0.21875 to 0.21875
Outputs:
- mixed_out: bfloat16 [32768, 2048], P(('dp', 'expert'))
The draws below stay inside these ranges and needn't reach their ends.
Inputs may be any that keep to these rules, and one draw needn't show every extreme that they name: `expert_ids`: each row names 8 different experts.
All inputs are finite; a program needn't handle non-finite values.
Results may differ from the reference program's by a relative error of at most 0.0095.
Values may be sent and summed in bfloat16 or wider, within the bound.
A program may use at most 64 MiB of HBM per device.

```python
import math
import jax
import jax.numpy as jnp
from jax import lax

D = 2048
FF = 768
TOP = 8
TOK_DEV = 128
EXPERTS = 128
SHARDS = 256
TOKENS = 32768
CAP = 8
COL_CAP = 128
N_DP = 32
N_EXPERT = 8


def draw_shard_limit(key, part):
    key_base = jax.random.fold_in(key, 11)
    key_full = jax.random.fold_in(key, 12)
    drawn_base = jax.random.randint(key_base, (SHARDS, EXPERTS), CAP // 2, CAP + 1)
    full_mark = jax.random.randint(key_full, (SHARDS, EXPERTS), 0, 2)
    return jnp.where(full_mark == 1, CAP, drawn_base).astype(jnp.int32)


def block_levels(key, extent, split, least, largest):
    factor_of = 1.0
    for dim, parts in split:
        heights = jax.random.uniform(jax.random.fold_in(jax.random.fold_in(key, 6), dim), (parts,), jnp.float32, least / len(split), largest / len(split))
        factor_of = factor_of * jnp.repeat(jnp.exp(heights), extent[dim] // parts).reshape((-1,) + (1,) * (len(extent) - 1 - dim))
    return factor_of


def choose_distinct(own_key, rows, number_of, top, lift):
    sequence = jax.random.permutation(jax.random.fold_in(own_key, 1), number_of)
    boost = sequence
    for power in range(3):
        boost = boost * boost // number_of
    boost = boost * lift // number_of
    lots = jax.random.randint(jax.random.fold_in(own_key, 2), (rows, number_of), 0, 4096) + boost
    sure = jax.random.permutation(jax.random.fold_in(own_key, 3), rows)[jnp.arange(number_of) % rows]
    lots = jnp.where(jnp.arange(rows)[:, None] == sure[None, :], 1 << 14, lots)
    merit = lots * number_of + jnp.arange(number_of)
    return lax.top_k(merit.astype(jnp.int32), top)[1].astype(jnp.int32)


def noise(own_key, shape, spread, most, split=(), held_as=jnp.bfloat16):
    factor_of = block_levels(own_key, shape, split, -0.22, 0.18) if split else 1.0
    values = jax.random.normal(own_key, shape, jnp.float32) * spread * factor_of
    return jnp.minimum(jnp.maximum(values, -most), most).astype(held_as)


def setup_inputs(seed: int = 0) -> dict:
    keys = jax.random.split(jax.random.key(seed), 8)
    return {
        "tokens": noise(keys[0], (TOKENS, D), 1.0, 6.0, ((0, 256),)),
        "expert_ids": choose_distinct(keys[1], TOKENS, EXPERTS, TOP, 1024),
        "route_probs": jnp.clip(jnp.exp(math.log(1.0) - 2.9957323 * jax.random.uniform(keys[2], (TOKENS, TOP), jnp.float32) ** block_levels(keys[2], (TOKENS, TOP), ((0, 256),), -0.2, 0.2)), 0.05, 1.0),
        "shard_limit": draw_shard_limit(jax.random.fold_in(keys[7], 71), 0),
        "gate_proj": noise(keys[4], (2 * EXPERTS, D, FF // 2), D ** -0.5, 0.125, ((0, 256),)),
        "up_proj": noise(keys[5], (2 * EXPERTS, D, FF // 2), D ** -0.5, 0.125, ((0, 256),)),
        "down_proj": noise(keys[6], (2 * EXPERTS, FF // 2, D), FF ** -0.5, 0.21875, ((0, 256),)),
    }


def half_pair(rows_in, gate_pair, up_pair, down_pair):
    partials = []
    for half_index in range(2):
        gate_val = jnp.dot(rows_in, gate_pair[half_index], preferred_element_type=jnp.float32)
        up_val = jnp.dot(rows_in, up_pair[half_index], preferred_element_type=jnp.float32)
        hidden = (jax.nn.silu(gate_val) * up_val).astype(jnp.bfloat16)
        partials.append(jnp.dot(hidden, down_pair[half_index], preferred_element_type=jnp.float32).astype(jnp.bfloat16))
    return (partials[0].astype(jnp.float32) + partials[1].astype(jnp.float32)).astype(jnp.bfloat16)


def expert_apply(packed):
    return half_pair(packed[0], packed[1], packed[2], packed[3])


def reference(tokens, expert_ids, route_probs, shard_limit, gate_proj, up_proj, down_proj):
    shards = N_DP * N_EXPERT
    route_ids = expert_ids.reshape(shards, TOK_DEV * TOP)
    onehot = (route_ids[:, :, None] == jnp.arange(EXPERTS, dtype=jnp.int32)[None, None, :]).astype(jnp.int32)
    before = (jnp.cumsum(onehot, axis=1) - onehot).astype(jnp.int32)
    slot_rank = jnp.sum(before * onehot, axis=2).astype(jnp.int32)
    expert_count = jnp.sum(onehot, axis=1).astype(jnp.int32)
    kept_count = jnp.minimum(expert_count, shard_limit)
    count_grid = kept_count.reshape(N_DP, N_EXPERT, EXPERTS)
    offset = (jnp.cumsum(count_grid, axis=0) - count_grid).astype(jnp.int32).reshape(shards, EXPERTS)
    limit_each = jnp.take_along_axis(shard_limit, route_ids, axis=1)
    offset_each = jnp.take_along_axis(offset, route_ids, axis=1)
    slot_global = offset_each + slot_rank
    kept_mask = (slot_rank < limit_each) & (slot_global < COL_CAP)
    column = (jnp.arange(shards, dtype=jnp.int32) % N_EXPERT)[:, None]
    per_expert = N_EXPERT * COL_CAP
    total_slots = EXPERTS * per_expert
    target = jnp.where(kept_mask, route_ids * per_expert + column * COL_CAP + slot_global, total_slots).astype(jnp.int32)
    target = target.reshape(shards * TOK_DEV, TOP)
    kept_rows = kept_mask.reshape(shards * TOK_DEV, TOP)
    buffers = jnp.zeros((total_slots, D), jnp.bfloat16)
    for choice_num in range(TOP):
        buffers = buffers.at[target[:, choice_num]].set(tokens, mode="drop")
    buffers = buffers.reshape(EXPERTS, per_expert, D)
    expert_rows = lax.map(expert_apply, (buffers, gate_proj.reshape(EXPERTS, 2, D, FF // 2), up_proj.reshape(EXPERTS, 2, D, FF // 2), down_proj.reshape(EXPERTS, 2, FF // 2, D)))
    flat_rows = expert_rows.reshape(total_slots, D)
    total = jnp.zeros((shards * TOK_DEV, D), jnp.float32)
    for choice_num in range(TOP):
        index_now = jnp.minimum(target[:, choice_num], total_slots - 1)
        fetched = flat_rows[index_now].astype(jnp.float32)
        weight = route_probs[:, choice_num] * kept_rows[:, choice_num].astype(jnp.float32)
        total = total + weight[:, None] * fetched
    return total.astype(jnp.bfloat16)
```

```python
import jax
import jax.numpy as jnp
from jax import lax
from jax.experimental import pallas as pl
from jax.experimental.pallas import tpu as pltpu
from jax.sharding import PartitionSpec as P

MESH = pl.DeviceIdType.MESH
BF = jnp.bfloat16
F32 = jnp.float32

NX, NY, NZ = 4, 4, 8
TOK = 128
SLOTS = 8
COL_CAP = 128
WIDTH = 2048
HALF = WIDTH // 2
HIDDEN = 768
PEERS = NX * NY
ROWS = PEERS * 2 * SLOTS
UNIT = 2 * SLOTS
EXPERTS = 128


def kernel(
    tokens, ids, probs, limit, gate, up, down, out,
    tok, meta, totals, gw, uw, dw, sbuf, rbuf, hid, obuf, ybuf, mix, part, own, rs_in, rs_out,
    in_sem, w_loc, w_send, w_recv, meta_send, meta_recv, tot_send, tot_recv,
    ag_send, ag_recv, d_send, d_recv, r_send, r_recv, rs_send, rs_recv,
):
    d = lax.axis_index("dp")
    c = lax.axis_index("expert")
    x, z = d // NZ, d % NZ
    y, core = c // 2, c % 2
    me = x * NY + y
    partner = (d, y * 2 + (1 - core))

    def z_peer(step):
        return (x * NZ + (z + step) % NZ, c)

    def xy_peer(i):
        px, py = (x + i % NX) % NX, (y + i // NX) % NY
        return px * NY + py, (px * NZ + z, py * 2 + core)

    def x_peer(i):
        return (((x + i) % NX) * NZ + z, c)

    def rows_of(chip):
        return pl.ds(pl.multiple_of(chip * UNIT, UNIT), UNIT)

    def remote(src, dst, send, recv, device):
        return pltpu.make_async_remote_copy(
            src_ref=src, dst_ref=dst, send_sem=send, recv_sem=recv,
            device_id=device, device_id_type=MESH,
        )

    for h in range(2):
        pltpu.make_async_copy(tokens.at[:, pl.ds(h * HALF, HALF)], tok.at[z, h], in_sem.at[h]).start()
    wide = pl.ds(pl.multiple_of(core * (HIDDEN // 2), HIDDEN // 2), HIDDEN // 2)
    weights = (
        (gate.at[0], gw.at[:, wide]), (up.at[0], uw.at[:, wide]), (down.at[0], dw.at[wide, :]),
    )
    for i, (src, dst) in enumerate(weights):
        pltpu.make_async_copy(src, dst, w_loc.at[i]).start()

    barrier = pltpu.get_barrier_semaphore()
    pl.semaphore_signal(barrier, inc=1, device_id=partner, device_id_type=MESH)

    def greet_z(i, carry):
        pl.semaphore_signal(barrier, inc=1, device_id=z_peer(i), device_id_type=MESH)
        return carry

    def greet_xy(i, carry):
        pl.semaphore_signal(barrier, inc=1, device_id=xy_peer(i)[1], device_id_type=MESH)
        return carry

    lax.fori_loop(1, NZ, greet_z, 0)
    lax.fori_loop(1, PEERS, greet_xy, 0)

    lane = lax.broadcasted_iota(jnp.int32, (TOK, EXPERTS), 1)
    row = lax.broadcasted_iota(jnp.int32, (TOK, EXPERTS), 0)
    chosen = jnp.zeros((TOK, EXPERTS), F32)
    weight = jnp.zeros((TOK, EXPERTS), F32)
    for k in range(8):
        hit = ids[:, k : k + 1] == lane
        chosen = jnp.where(hit, 1.0, chosen)
        weight = jnp.where(hit, probs[:, k : k + 1], weight)
    earlier = jnp.where(lane < row, 1.0, 0.0).astype(BF)
    rank = jnp.dot(earlier, chosen.astype(BF), preferred_element_type=F32)
    rank = jnp.where((chosen > 0.5) & (rank < limit[...].astype(F32)), rank, 1000.0)
    row_f = row.astype(F32)
    for r in range(SLOTS):
        at = rank == float(r)
        meta[z, r : r + 1, :] = jnp.sum(jnp.where(at, row_f + 1000.0, 0.0), axis=0, keepdims=True) - 1000.0
        meta[z, SLOTS + r : SLOTS + r + 1, :] = jnp.sum(jnp.where(at, weight, 0.0), axis=0, keepdims=True)

    pl.semaphore_wait(barrier, NZ - 1 + PEERS - 1 + 1)

    def ag(way, hop, h):
        block = (z + NZ - hop + 1) % NZ if way == 0 else (z + hop - 1) % NZ
        return remote(
            tok.at[block, h], tok.at[block, h], ag_send.at[way, hop - 1, h], ag_recv.at[way, hop - 1, h],
            z_peer(1 if way == 0 else NZ - 1),
        )

    def ag_arrival(way, hop, h):
        block = (z + NZ - hop) % NZ if way == 0 else (z + hop) % NZ
        return remote(
            tok.at[block, h], tok.at[block, h], ag_send.at[way, hop - 1, h], ag_recv.at[way, hop - 1, h],
            z_peer(1 if way == 0 else NZ - 1),
        )

    for h in range(2):
        pltpu.make_async_copy(tokens.at[:, pl.ds(h * HALF, HALF)], tok.at[z, h], in_sem.at[h]).wait()
        for way in range(2):
            ag(way, 1, h).start()

    def send_meta(i, carry):
        remote(meta.at[z], meta.at[z], meta_send, meta_recv, z_peer(i)).start()
        return carry

    lax.fori_loop(1, NZ, send_meta, 0)
    for i, (src, dst) in enumerate(weights):
        remote(src, dst, w_send.at[i], w_recv.at[i], partner).start()

    several = meta.at[pl.ds(0, NZ - 1)]
    remote(several, several, meta_send, meta_recv, z_peer(1)).wait_recv()

    total = jnp.zeros((1, EXPERTS), F32)
    for s in range(NZ):
        total = total + jnp.sum(jnp.where(meta[s, 0:SLOTS, :] >= 0.0, 1.0, 0.0), axis=0, keepdims=True)
    totals[x] = jnp.broadcast_to(total, (8, EXPERTS))

    def send_total(i, carry):
        remote(totals.at[x], totals.at[x], tot_send, tot_recv, x_peer(i)).start()
        return carry

    lax.fori_loop(1, NX, send_total, 0)

    def pair(g):
        return (z + NZ - g - 1) % NZ, (z + (g + 1) % 4) % NZ

    def slot_values(first, second):
        stacked = jnp.concatenate([first, second] * PEERS, axis=0)
        s = lax.broadcasted_iota(jnp.int32, (ROWS, EXPERTS), 0)
        e = lax.broadcasted_iota(jnp.int32, (ROWS, EXPERTS), 1)
        chip = s >> 4
        expert = (chip >> 2) * (NZ * NY) + z * NY + (chip & 3)
        return jnp.sum(jnp.where(e == expert, stacked, 0.0), axis=1, keepdims=True)

    def selection(g):
        a, b = pair(g)
        source = slot_values(meta[a, 0:SLOTS, :], meta[b, 0:SLOTS, :])
        s = lax.broadcasted_iota(jnp.int32, (ROWS, 2 * TOK), 0)
        t = lax.broadcasted_iota(jnp.int32, (ROWS, 2 * TOK), 1)
        second = (s >> 3) & 1
        return (t - second * TOK).astype(F32) == source

    def exchange(src, dst, send, recv, g, h):
        def one(i, carry):
            chip, device = xy_peer(i)
            remote(src.at[g, h, rows_of(chip)], dst.at[g, h, rows_of(me)], send.at[g, h], recv.at[g, h], device).start()
            return carry

        lax.fori_loop(1, PEERS, one, 0)

    def exchanged(src, dst, send, recv, g, h):
        most = pl.ds(0, (PEERS - 1) * UNIT)
        return remote(src.at[g, h, most], dst.at[g, h, most], send.at[g, h], recv.at[g, h], x_peer(1))

    def dispatch(g):
        a, b = pair(g)
        pick = jnp.where(selection(g), 1.0, 0.0).astype(BF)
        for h in range(2):
            for way in range(2):
                def arrive(way=way, h=h):
                    ag_arrival(way, g + 1, h).wait_recv()

                def forward(way=way, h=h):
                    ag(way, g + 2, h).start()

                if way == h:
                    arrive()
                    pl.when(g < 3)(forward)
                else:
                    pl.when(g < 3)(arrive)
                    pl.when(g < 2)(forward)
            for n in range(0, HALF, 512):
                both = jnp.concatenate([tok[a, h, :, n : n + 512], tok[b, h, :, n : n + 512]], axis=0)
                sbuf[g, h, :, n : n + 512] = jnp.dot(pick, both, preferred_element_type=F32).astype(BF)
            exchange(sbuf, rbuf, d_send, d_recv, g, h)
            rbuf[g, h, rows_of(me), :] = sbuf[g, h, rows_of(me), :]

    def feed_forward(g):
        for h in range(2):
            exchanged(sbuf, rbuf, d_send, d_recv, g, h).wait_recv()
        for n in range(0, HIDDEN, 256):
            cols = slice(n, n + 256)
            gv = jnp.dot(rbuf[g, 0], gw[0:HALF, cols], preferred_element_type=F32)
            gv = gv + jnp.dot(rbuf[g, 1], gw[HALF:WIDTH, cols], preferred_element_type=F32)
            uv = jnp.dot(rbuf[g, 0], uw[0:HALF, cols], preferred_element_type=F32)
            uv = uv + jnp.dot(rbuf[g, 1], uw[HALF:WIDTH, cols], preferred_element_type=F32)
            hid[:, cols] = (gv / (1.0 + jnp.exp(-gv)) * uv).astype(BF)
        for h in range(2):
            for n in range(0, HALF, 256):
                obuf[g, h, :, n : n + 256] = jnp.dot(
                    hid[...], dw[:, h * HALF + n : h * HALF + n + 256], preferred_element_type=F32
                ).astype(BF)
            ybuf[g, h, rows_of(me), :] = obuf[g, h, rows_of(me), :]

    for i, (src, dst) in enumerate(weights):
        pltpu.make_async_copy(src, dst, w_loc.at[i]).wait()
    other = pl.ds(pl.multiple_of((1 - core) * (HIDDEN // 2), HIDDEN // 2), HIDDEN // 2)
    theirs = (gw.at[:, other], uw.at[:, other], dw.at[other, :])

    def step(g, carry):
        pl.when(g < 4)(lambda: dispatch(g))

        @pl.when(g == 1)
        def _():
            for i, (src, _) in enumerate(weights):
                remote(src, theirs[i], w_send.at[i], w_recv.at[i], partner).wait_recv()

        pl.when(g > 0)(lambda: feed_forward(g - 1))
        return carry

    lax.fori_loop(0, 5, step, 0)

    for h in range(2):
        exchange(obuf, ybuf, r_send, r_recv, 3, h)

    some = totals.at[pl.ds(0, NX - 1)]
    remote(some, some, tot_send, tot_recv, x_peer(1)).wait_recv()
    before_x = jnp.zeros((1, EXPERTS), F32)
    for s in range(NX):
        before_x = before_x + jnp.where(s < x, 1.0, 0.0) * totals[s, 0:1, :]

    def kept_weight(shard):
        offset = before_x
        for s in range(NZ):
            count = jnp.sum(jnp.where(meta[s, 0:SLOTS, :] >= 0.0, 1.0, 0.0), axis=0, keepdims=True)
            offset = offset + jnp.where(s < shard, 1.0, 0.0) * count
        r = lax.broadcasted_iota(jnp.int32, (SLOTS, EXPERTS), 0).astype(F32)
        return jnp.where(offset + r < float(COL_CAP), meta[shard, SLOTS : 2 * SLOTS, :], 0.0)

    def mixing(g):
        a, b = pair(g)
        w = slot_values(kept_weight(a), kept_weight(b))
        mix[g] = jnp.where(selection(g), w, 0.0).T.astype(BF)

    def mix_step(g, carry):
        mixing(g)
        return carry

    lax.fori_loop(0, 4, mix_step, 0)

    def rs(way, g, h):
        return remote(
            rs_out.at[way, g, h], rs_in.at[way, g, h], rs_send.at[way, g, h], rs_recv.at[way, g, h],
            z_peer(1 if way == 0 else NZ - 1),
        )

    def collect(i, carry):
        g = 3 - i

        @pl.when(g > 0)
        def _():
            for h in range(2):
                exchange(obuf, ybuf, r_send, r_recv, g - 1, h)

        for h in range(2):
            exchanged(obuf, ybuf, r_send, r_recv, g, h).wait_recv()
            for n in range(0, HALF, 512):
                part[:, n : n + 512] = jnp.dot(mix[g], ybuf[g, h, :, n : n + 512], preferred_element_type=F32)

            @pl.when(g == 3)
            def _():
                own[h] = part[TOK : 2 * TOK, :]
                rs_out[h, 3, h] = part[0:TOK, :].astype(BF)
                rs(h, 3, h).start()

            @pl.when(g < 3)
            def _():
                for way in range(2):
                    mine = slice(TOK, 2 * TOK) if way == 0 else slice(0, TOK)

                    def add(way=way, mine=mine):
                        rs(way, g + 1, h).wait_recv()
                        rs_out[way, g, h] = (part[mine, :] + rs_in[way, g + 1, h].astype(F32)).astype(BF)

                    def first(way=way, mine=mine):
                        rs_out[way, g, h] = part[mine, :].astype(BF)

                    if way == h:
                        add()
                    else:
                        pl.when(g < 2)(add)
                        pl.when(g == 2)(first)
                    rs(way, g, h).start()

        return carry

    lax.fori_loop(0, 4, collect, 0)

    for h in range(2):
        for way in range(2):
            rs(way, 0, h).wait_recv()
        out[:, h * HALF : (h + 1) * HALF] = (
            own[h] + rs_in[0, 0, h].astype(F32) + rs_in[1, 0, h].astype(F32)
        ).astype(BF)

    for i, (src, dst) in enumerate(weights):
        remote(src, dst, w_send.at[i], w_recv.at[i], partner).wait_send()
    remote(several, several, meta_send, meta_recv, z_peer(1)).wait_send()
    remote(some, some, tot_send, tot_recv, x_peer(1)).wait_send()
    for g in range(4):
        for h in range(2):
            exchanged(sbuf, rbuf, d_send, d_recv, g, h).wait_send()
            exchanged(obuf, ybuf, r_send, r_recv, g, h).wait_send()
            for way in range(2):
                if g < 3 or way == h:
                    ag(way, g + 1, h).wait_send()
                    rs(way, g, h).wait_send()


def on_device(tokens, expert_ids, route_probs, shard_limit, gate_proj, up_proj, down_proj):
    dma = pltpu.SemaphoreType.DMA
    anywhere = pl.BlockSpec(memory_space=pl.ANY)
    near = pl.BlockSpec(memory_space=pltpu.VMEM)
    return pl.pallas_call(
        kernel,
        out_shape=jax.ShapeDtypeStruct((TOK, WIDTH), BF),
        in_specs=[anywhere, near, near, near, anywhere, anywhere, anywhere],
        out_specs=near,
        scratch_shapes=[
            pltpu.VMEM((NZ, 2, TOK, HALF), BF),
            pltpu.VMEM((NZ, 2 * SLOTS, EXPERTS), F32),
            pltpu.VMEM((NX, 8, EXPERTS), F32),
            pltpu.VMEM((WIDTH, HIDDEN), BF),
            pltpu.VMEM((WIDTH, HIDDEN), BF),
            pltpu.VMEM((HIDDEN, WIDTH), BF),
            pltpu.VMEM((4, 2, ROWS, HALF), BF),
            pltpu.VMEM((4, 2, ROWS, HALF), BF),
            pltpu.VMEM((ROWS, HIDDEN), BF),
            pltpu.VMEM((4, 2, ROWS, HALF), BF),
            pltpu.VMEM((4, 2, ROWS, HALF), BF),
            pltpu.VMEM((4, 2 * TOK, ROWS), BF),
            pltpu.VMEM((2 * TOK, HALF), F32),
            pltpu.VMEM((2, TOK, HALF), F32),
            pltpu.VMEM((2, 4, 2, TOK, HALF), BF),
            pltpu.VMEM((2, 4, 2, TOK, HALF), BF),
            dma((2,)), dma((3,)), dma((3,)), dma((3,)), dma, dma, dma, dma,
            dma((2, 4, 2)), dma((2, 4, 2)), dma((4, 2)), dma((4, 2)), dma((4, 2)), dma((4, 2)),
            dma((2, 4, 2)), dma((2, 4, 2)),
        ],
        compiler_params=pltpu.CompilerParams(
            collective_id=0, has_side_effects=True, vmem_limit_bytes=60 * 1024 * 1024
        ),
        name="expert_layer",
    )(tokens, expert_ids, route_probs, shard_limit, gate_proj, up_proj, down_proj)


def solution(mesh):
    whole = ("dp", "expert")
    in_specs = (
        P(whole, None), P(whole, None), P(whole, None), P(whole, None),
        P(whole, None, None), P(whole, None, None), P(whole, None, None),
    )
    return jax.shard_map(
        on_device, mesh=mesh, in_specs=in_specs, out_specs=P(whole, None), check_vma=False
    )
```

```python
import jax
import jax.numpy as jnp
from jax import lax
from jax.experimental import pallas as pl
from jax.experimental.pallas import tpu as pltpu
from jax.sharding import PartitionSpec as P

MESH = pl.DeviceIdType.MESH
BF = jnp.bfloat16
F32 = jnp.float32

NX, NY, NZ = 4, 4, 8
TOK = 128
SLOTS = 8
COL_CAP = 128
WIDTH = 2048
CHUNKS = 4
COLS = WIDTH // CHUNKS
HIDDEN = 768
PEERS = NX * NY
UNIT = 2 * SLOTS
ROWS = PEERS * UNIT
EXPERTS = 128
FAR = NZ // 2
UP, DOWN = 0, 1


def kernel(
    tokens, ids, probs, limit, gate, up, down, out,
    tok, meta, totals, gw, uw, dw, sbuf, rbuf, hid, obuf, ybuf, mix, part, rs_in, rs_out,
    in_sem, w_loc, w_send, w_recv, meta_send, meta_recv, tot_send, tot_recv,
    ag_send, ag_recv, d_send, d_recv, r_send, r_recv, rs_send, rs_recv,
):
    d = lax.axis_index("dp")
    c_all = lax.axis_index("expert")
    x, z = d // NZ, d % NZ
    y, core = c_all // 2, c_all % 2
    me = x * NY + y
    partner = (d, y * 2 + (1 - core))

    def z_peer(step):
        return (x * NZ + (z + step) % NZ, c_all)

    def neighbour(way):
        return z_peer(1 if way == UP else NZ - 1)

    def xy_peer(i):
        px, py = (x + i % NX) % NX, (y + i // NX) % NY
        return px * NY + py, (px * NZ + z, py * 2 + core)

    def x_peer(i):
        return (((x + i) % NX) * NZ + z, c_all)

    def rows_of(chip):
        return pl.ds(pl.multiple_of(chip * UNIT, UNIT), UNIT)

    def remote(src, dst, send, recv, device):
        return pltpu.make_async_remote_copy(
            src_ref=src, dst_ref=dst, send_sem=send, recv_sem=recv,
            device_id=device, device_id_type=MESH,
        )

    def own_tokens(c):
        return pltpu.make_async_copy(tokens.at[:, pl.ds(c * COLS, COLS)], tok.at[z, c], in_sem.at[c])

    for c in range(CHUNKS):
        own_tokens(c).start()
    wide = pl.ds(pl.multiple_of(core * (HIDDEN // 2), HIDDEN // 2), HIDDEN // 2)
    other = pl.ds(pl.multiple_of((1 - core) * (HIDDEN // 2), HIDDEN // 2), HIDDEN // 2)
    weights = (
        (gate.at[0], gw.at[:, wide]), (up.at[0], uw.at[:, wide]), (down.at[0], dw.at[wide, :]),
    )
    theirs = (gw.at[:, other], uw.at[:, other], dw.at[other, :])
    for i, (src, dst) in enumerate(weights):
        pltpu.make_async_copy(src, dst, w_loc.at[i]).start()

    barrier = pltpu.get_barrier_semaphore()
    pl.semaphore_signal(barrier, inc=1, device_id=partner, device_id_type=MESH)

    def greet_z(i, carry):
        pl.semaphore_signal(barrier, inc=1, device_id=z_peer(i), device_id_type=MESH)
        return carry

    def greet_xy(i, carry):
        pl.semaphore_signal(barrier, inc=1, device_id=xy_peer(i)[1], device_id_type=MESH)
        return carry

    lax.fori_loop(1, NZ, greet_z, 0)
    lax.fori_loop(1, PEERS, greet_xy, 0)

    col = lax.broadcasted_iota(jnp.int32, (EXPERTS, TOK), 1)
    row = lax.broadcasted_iota(jnp.int32, (EXPERTS, TOK), 0)
    chosen = jnp.zeros((EXPERTS, TOK), F32)
    weight = jnp.zeros((EXPERTS, TOK), F32)
    for k in range(8):
        hit = ids[k : k + 1, :] == row
        chosen = jnp.where(hit, 1.0, chosen)
        weight = jnp.where(hit, probs[k : k + 1, :], weight)
    earlier = jnp.where(row < col, 1.0, 0.0).astype(BF)
    rank = jnp.dot(chosen.astype(BF), earlier, preferred_element_type=F32)
    rank = jnp.where(chosen > 0.5, rank, 1000.0).T
    weight = weight.T
    rank = jnp.where(rank < limit[...].astype(F32), rank, 1000.0)
    token_id = row.astype(F32)
    for r in range(SLOTS):
        at = rank == float(r)
        meta[z, r : r + 1, :] = jnp.sum(jnp.where(at, token_id + 1000.0, 0.0), axis=0, keepdims=True) - 1000.0
        meta[z, SLOTS + r : SLOTS + r + 1, :] = jnp.sum(jnp.where(at, weight, 0.0), axis=0, keepdims=True)

    pl.semaphore_wait(barrier, NZ - 1 + PEERS - 1 + 1)

    def send_meta(i, carry):
        remote(meta.at[z], meta.at[z], meta_send, meta_recv, z_peer(i)).start()
        return carry

    lax.fori_loop(1, NZ, send_meta, 0)

    def ag(way, hop, c):
        block = (z + NZ - hop + 1) % NZ if way == UP else (z + hop - 1) % NZ
        return remote(
            tok.at[block, c], tok.at[block, c], ag_send.at[way, hop - 1, c], ag_recv.at[way, hop - 1, c],
            neighbour(way),
        )

    def ag_arrival(way, hop, c):
        block = (z + NZ - hop) % NZ if way == UP else (z + hop) % NZ
        return remote(
            tok.at[block, c], tok.at[block, c], ag_send.at[way, hop - 1, c], ag_recv.at[way, hop - 1, c],
            neighbour(way),
        )

    for c in range(CHUNKS):
        own_tokens(c).wait()
        for way in range(2):
            ag(way, 1, c).start()
    for i, (src, dst) in enumerate(weights):
        remote(src, dst, w_send.at[i], w_recv.at[i], partner).start()

    def metas():
        several = meta.at[pl.ds(0, NZ - 1)]
        return remote(several, several, meta_send, meta_recv, z_peer(1))

    def some_totals():
        some = totals.at[pl.ds(0, NX - 1)]
        return remote(some, some, tot_send, tot_recv, x_peer(1))

    def count_of(s):
        return jnp.sum(jnp.where(meta[s, 0:SLOTS, :] >= 0.0, 1.0, 0.0), axis=0, keepdims=True)

    def send_totals():
        total = jnp.zeros((1, EXPERTS), F32)
        for s in range(NZ):
            total = total + count_of(s)
        totals[x] = jnp.broadcast_to(total, (8, EXPERTS))

        def send_total(i, carry):
            remote(totals.at[x], totals.at[x], tot_send, tot_recv, x_peer(i)).start()
            return carry

        lax.fori_loop(1, NX, send_total, 0)

    def pair(k):
        return (z + NZ - k) % NZ, (z + k) % NZ

    def far_chunk(k, c):
        return c + 2 * (1 - (k % 4 + 3) // 4)

    def slot_values(first, second):
        stacked = jnp.concatenate([first, second] * PEERS, axis=0)
        s = lax.broadcasted_iota(jnp.int32, (ROWS, EXPERTS), 0)
        e = lax.broadcasted_iota(jnp.int32, (ROWS, EXPERTS), 1)
        chip = s >> 4
        expert = (chip >> 2) * (NZ * NY) + z * NY + (chip & 3)
        return jnp.sum(jnp.where(e == expert, stacked, 0.0), axis=1, keepdims=True)

    def selection(k):
        a, b = pair(k)
        source = slot_values(meta[a, 0:SLOTS, :], meta[b, 0:SLOTS, :])
        s = lax.broadcasted_iota(jnp.int32, (ROWS, 2 * TOK), 0)
        t = lax.broadcasted_iota(jnp.int32, (ROWS, 2 * TOK), 1)
        second = (s >> 3) & 1
        return (t - second * TOK).astype(F32) == source

    def exchange(src, dst, send, recv, k, c):
        def one(i, carry):
            chip, device = xy_peer(i)
            remote(src.at[k, c, rows_of(chip)], dst.at[k, c, rows_of(me)], send.at[k, c], recv.at[k, c], device).start()
            return carry

        lax.fori_loop(1, PEERS, one, 0)

    def exchanged(src, dst, send, recv, k, c):
        most = pl.ds(0, (PEERS - 1) * UNIT)
        return remote(src.at[k, c, most], dst.at[k, c, most], send.at[k, c], recv.at[k, c], x_peer(1))

    def dispatch(k, c):
        a, b = pair(k)
        c_b = far_chunk(k, c)

        def arrive_up():
            ag_arrival(UP, k, c).wait_recv()

        def arrive_down():
            ag_arrival(DOWN, k, c_b).wait_recv()

        if c < 2:
            pl.when(k > 0)(arrive_up)
            pl.when((k > 0) & (k < FAR))(lambda: ag(UP, k + 1, c).start())
            pl.when(k > 0)(arrive_down)
            pl.when((k > 0) & (k < FAR - 1))(lambda: ag(DOWN, k + 1, c).start())
        else:
            arrive_up()
            pl.when(k < FAR - 1)(lambda: ag(UP, k + 1, c).start())
            arrive_down()
            ag(DOWN, k + 1, c).start()
        both = jnp.concatenate([tok[a, c], tok[b, c_b]], axis=0)
        sbuf[k, c] = jnp.dot(mix[k], both, preferred_element_type=F32).astype(BF)
        exchange(sbuf, rbuf, d_send, d_recv, k, c)
        rbuf[k, c, rows_of(me), :] = sbuf[k, c, rows_of(me), :]

    second_half = (lax.broadcasted_iota(jnp.int32, (ROWS, 256), 0) >> 3) & 1
    second_wide = (lax.broadcasted_iota(jnp.int32, (ROWS, COLS), 0) >> 3) & 1

    def block(c):
        return slice(c * COLS, (c + 1) * COLS)

    def split_k(k):
        return (k > 0) & (k < FAR)

    def hidden(k, n):
        cols = slice(n * 256, (n + 1) * 256)

        def product(chunk, w, rows):
            return jnp.dot(rbuf[k, chunk], w[block(rows), cols], preferred_element_type=F32)

        def finish(gv, uv):
            hid[:, cols] = (gv / (1.0 + jnp.exp(-gv)) * uv).astype(BF)

        @pl.when(split_k(k))
        def _():
            finish(*(sum(product(c, w, c) for c in range(CHUNKS)) for w in (gw, uw)))

        @pl.when(jnp.logical_not(split_k(k)))
        def _():
            sums = []
            for w in (gw, uw):
                left = product(0, w, 0) + product(1, w, 1)
                right = product(0, w, 2) + product(1, w, 3)
                half = jnp.where(second_half == 0, left, right)
                swapped = jnp.where(
                    second_half == 0, pltpu.roll(half, ROWS - SLOTS, 0), pltpu.roll(half, SLOTS, 0)
                )
                sums.append(half + swapped)
            finish(*sums)

    def wait_rows(k):
        for c in range(2):
            exchanged(sbuf, rbuf, d_send, d_recv, k, c).wait_recv()

        @pl.when(split_k(k))
        def _():
            for c in range(2, CHUNKS):
                exchanged(sbuf, rbuf, d_send, d_recv, k, c).wait_recv()

    def outputs(k):
        def product(c):
            return jnp.dot(hid[...], dw[:, block(c)], preferred_element_type=F32)

        def keep(c, value):
            obuf[k, c] = value.astype(BF)
            ybuf[k, c, rows_of(me), :] = obuf[k, c, rows_of(me), :]

        @pl.when(split_k(k))
        def _():
            for c in range(CHUNKS):
                keep(c, product(c))

        @pl.when(jnp.logical_not(split_k(k)))
        def _():
            for c in range(2):
                keep(c, jnp.where(second_wide == 0, product(c), product(c + 2)))

    def weights_here():
        for i, (src, dst) in enumerate(weights):
            pltpu.make_async_copy(src, dst, w_loc.at[i]).wait()
            remote(src, theirs[i], w_send.at[i], w_recv.at[i], partner).wait_recv()

    def send_back(k):
        for c in range(2):
            exchange(obuf, ybuf, r_send, r_recv, k, c)

        @pl.when(split_k(k))
        def _():
            for c in range(2, CHUNKS):
                exchange(obuf, ybuf, r_send, r_recv, k, c)

    def weigh_all():
        some_totals().wait_recv()
        before_x = jnp.zeros((1, EXPERTS), F32)
        for s in range(NX):
            before_x = before_x + jnp.where(s < x, 1.0, 0.0) * totals[s, 0:1, :]

        def kept_weight(shard):
            offset = before_x
            for s in range(NZ):
                offset = offset + jnp.where(s < shard, 1.0, 0.0) * count_of(s)
            r = lax.broadcasted_iota(jnp.int32, (SLOTS, EXPERTS), 0).astype(F32)
            return jnp.where(offset + r < float(COL_CAP), meta[shard, SLOTS : 2 * SLOTS, :], 0.0)

        def weigh(k, carry):
            a, b = pair(k)
            w = slot_values(kept_weight(a), kept_weight(b))
            mix[k] = jnp.where(selection(k), w, 0.0).T.astype(BF)
            return carry

        lax.fori_loop(0, FAR + 1, weigh, 0)

    def step(k, carry):
        @pl.when(k == 1)
        def _():
            metas().wait_recv()
            send_totals()

        @pl.when(k <= FAR)
        def _():
            mix[k] = jnp.where(selection(k), 1.0, 0.0).astype(BF)

        for c in range(CHUNKS):
            if c < 2:
                pl.when(k <= FAR)(lambda: dispatch(k, c))
            else:
                pl.when(split_k(k))(lambda: dispatch(k, c))
            if c == 0:
                pl.when(k > 1)(lambda: hidden(k - 2, 2))
            if c == 1:
                pl.when(k > 1)(lambda: outputs(k - 2))
            if c == 2:
                pl.when(k == FAR + 1)(weigh_all)
                pl.when(k == 1)(weights_here)

                @pl.when((k > 0) & (k < FAR + 2))
                def _():
                    wait_rows(k - 1)
                    hidden(k - 1, 0)

            if c == 3:
                pl.when((k > 0) & (k < FAR + 2))(lambda: hidden(k - 1, 1))
        return carry

    lax.fori_loop(0, FAR + 3, step, 0)
    send_back(FAR)

    def rs(way, k, c):
        return remote(
            rs_out.at[way, k - 1, c], rs_in.at[way, k - 1, c], rs_send.at[way, k - 1, c], rs_recv.at[way, k - 1, c],
            neighbour(way),
        )

    def gather_part(k, c):
        exchanged(obuf, ybuf, r_send, r_recv, k, c).wait_recv()
        part[...] = jnp.dot(mix[k], ybuf[k, c], preferred_element_type=F32)

    def collect(i, carry):
        k = FAR - i
        send_back(k - 1)

        @pl.when(k == FAR)
        def _():
            for c in range(2):
                gather_part(k, c)
                for way in range(2):
                    rs_out[way, FAR - 1, c + 2 * way] = part[way * TOK : (way + 1) * TOK, :].astype(BF)
                    rs(way, FAR, c + 2 * way).start()

        @pl.when(k < FAR)
        def _():
            for c in range(CHUNKS):
                gather_part(k, c)
                for way in range(2):
                    mine = slice(TOK, 2 * TOK) if way == UP else slice(0, TOK)

                    def add(way=way, mine=mine):
                        rs(way, k + 1, c).wait_recv()
                        rs_out[way, k - 1, c] = (part[mine, :] + rs_in[way, k, c].astype(F32)).astype(BF)

                    def first(way=way, mine=mine):
                        rs_out[way, k - 1, c] = part[mine, :].astype(BF)

                    if c // 2 == way:
                        add()
                    else:
                        pl.when(k < FAR - 1)(add)
                        pl.when(k == FAR - 1)(first)
                    rs(way, k, c).start()

        return carry

    lax.fori_loop(0, FAR, collect, 0)

    for c in range(2):
        gather_part(0, c)
        for q in range(2):
            chunk = c + 2 * q
            for way in range(2):
                rs(way, 1, chunk).wait_recv()
            out[:, block(chunk)] = (
                part[q * TOK : (q + 1) * TOK, :] + rs_in[UP, 0, chunk].astype(F32) + rs_in[DOWN, 0, chunk].astype(F32)
            ).astype(BF)

    for i, (src, dst) in enumerate(weights):
        remote(src, dst, w_send.at[i], w_recv.at[i], partner).wait_send()
    metas().wait_send()
    some_totals().wait_send()
    for k in range(FAR + 1):
        for c in range(CHUNKS if 0 < k < FAR else 2):
            exchanged(sbuf, rbuf, d_send, d_recv, k, c).wait_send()
            exchanged(obuf, ybuf, r_send, r_recv, k, c).wait_send()
    for hop in range(1, FAR + 1):
        for c in range(CHUNKS):
            for way in range(2):
                if hop < FAR or c // 2 == way:
                    ag(way, hop, c).wait_send()
                    rs(way, hop, c).wait_send()


def on_device(tokens, expert_ids, route_probs, shard_limit, gate_proj, up_proj, down_proj):
    dma = pltpu.SemaphoreType.DMA
    anywhere = pl.BlockSpec(memory_space=pltpu.HBM)
    near = pl.BlockSpec(memory_space=pltpu.VMEM)
    unit = (FAR + 1, CHUNKS, ROWS, COLS)
    ring = (2, FAR, CHUNKS)
    return pl.pallas_call(
        kernel,
        out_shape=jax.ShapeDtypeStruct((TOK, WIDTH), BF),
        in_specs=[anywhere, near, near, near, anywhere, anywhere, anywhere],
        out_specs=near,
        scratch_shapes=[
            pltpu.VMEM((NZ, CHUNKS, TOK, COLS), BF),
            pltpu.VMEM((NZ, 2 * SLOTS, EXPERTS), F32),
            pltpu.VMEM((NX, 8, EXPERTS), F32),
            pltpu.VMEM((WIDTH, HIDDEN), BF),
            pltpu.VMEM((WIDTH, HIDDEN), BF),
            pltpu.VMEM((HIDDEN, WIDTH), BF),
            pltpu.VMEM(unit, BF),
            pltpu.VMEM(unit, BF),
            pltpu.VMEM((ROWS, HIDDEN), BF),
            pltpu.VMEM(unit, BF),
            pltpu.VMEM(unit, BF),
            pltpu.VMEM((FAR + 1, 2 * TOK, ROWS), BF),
            pltpu.VMEM((2 * TOK, COLS), F32),
            pltpu.VMEM((*ring, TOK, COLS), BF),
            pltpu.VMEM((*ring, TOK, COLS), BF),
            dma((CHUNKS,)), dma((3,)), dma((3,)), dma((3,)), dma, dma, dma, dma,
            dma(ring), dma(ring),
            dma(unit[:2]), dma(unit[:2]), dma(unit[:2]), dma(unit[:2]),
            dma(ring), dma(ring),
        ],
        compiler_params=pltpu.CompilerParams(
            collective_id=0, has_side_effects=True, vmem_limit_bytes=60000000
        ),
        name="expert_layer",
    )(tokens, expert_ids.T, route_probs.T, shard_limit, gate_proj, up_proj, down_proj)


def solution(mesh):
    whole = ("dp", "expert")
    in_specs = (
        P(whole, None), P(whole, None), P(whole, None), P(whole, None),
        P(whole, None, None), P(whole, None, None), P(whole, None, None),
    )
    return jax.shard_map(
        on_device, mesh=mesh, in_specs=in_specs, out_specs=P(whole, None), check_vma=False
    )
```

```python
import jax
import jax.numpy as jnp
from jax import lax
from jax.experimental import pallas as pl
from jax.experimental.pallas import tpu as pltpu
from jax.sharding import PartitionSpec as P

MESH = pl.DeviceIdType.MESH
BF = jnp.bfloat16
F32 = jnp.float32

NX, NY, NZ = 4, 4, 8
TOK = 128
SLOTS = 8
COL_CAP = 128
WIDTH = 2048
CHUNKS = 4
COLS = WIDTH // CHUNKS
HIDDEN = 768
PEERS = NX * NY
UNIT = 2 * SLOTS
ROWS = PEERS * UNIT
EXPERTS = 128
FAR = NZ // 2
UP, DOWN = 0, 1


def kernel(
    tokens, ids, probs, limit, gate, up, down, out,
    tok, meta, totals, gw, uw, dw, sbuf, rbuf, hid, obuf, ybuf, mix, part, held, rs_in, rs_out,
    in_sem, w_loc, w_send, w_recv, meta_send, meta_recv, tot_send, tot_recv,
    ag_send, ag_recv, d_send, d_recv, r_send, r_recv, rs_send, rs_recv,
):
    d = lax.axis_index("dp")
    c_all = lax.axis_index("expert")
    x, z = d // NZ, d % NZ
    y, core = c_all // 2, c_all % 2
    me = x * NY + y
    partner = (d, y * 2 + (1 - core))

    def z_peer(step):
        return (x * NZ + (z + step) % NZ, c_all)

    def neighbour(way):
        return z_peer(1 if way == UP else NZ - 1)

    def xy_peer(i):
        px, py = (x + i % NX) % NX, (y + i // NX) % NY
        return px * NY + py, (px * NZ + z, py * 2 + core)

    def x_peer(i):
        return (((x + i) % NX) * NZ + z, c_all)

    def rows_of(chip):
        return pl.ds(pl.multiple_of(chip * UNIT, UNIT), UNIT)

    def remote(src, dst, send, recv, device):
        return pltpu.make_async_remote_copy(
            src_ref=src, dst_ref=dst, send_sem=send, recv_sem=recv,
            device_id=device, device_id_type=MESH,
        )

    def own_tokens(c):
        return pltpu.make_async_copy(tokens.at[:, pl.ds(c * COLS, COLS)], tok.at[z, c], in_sem.at[c])

    for c in range(CHUNKS):
        own_tokens(c).start()
    wide = pl.ds(pl.multiple_of(core * (HIDDEN // 2), HIDDEN // 2), HIDDEN // 2)
    other = pl.ds(pl.multiple_of((1 - core) * (HIDDEN // 2), HIDDEN // 2), HIDDEN // 2)
    weights = (
        (gate.at[0], gw.at[:, wide]), (up.at[0], uw.at[:, wide]), (down.at[0], dw.at[wide, :]),
    )
    theirs = (gw.at[:, other], uw.at[:, other], dw.at[other, :])
    for i, (src, dst) in enumerate(weights):
        pltpu.make_async_copy(src, dst, w_loc.at[i]).start()

    barrier = pltpu.get_barrier_semaphore()
    pl.semaphore_signal(barrier, inc=1, device_id=partner, device_id_type=MESH)

    def greet_z(i, carry):
        pl.semaphore_signal(barrier, inc=1, device_id=z_peer(i), device_id_type=MESH)
        return carry

    def greet_xy(i, carry):
        pl.semaphore_signal(barrier, inc=1, device_id=xy_peer(i)[1], device_id_type=MESH)
        return carry

    lax.fori_loop(1, NZ, greet_z, 0)
    lax.fori_loop(1, PEERS, greet_xy, 0)

    col = lax.broadcasted_iota(jnp.int32, (EXPERTS, TOK), 1)
    row = lax.broadcasted_iota(jnp.int32, (EXPERTS, TOK), 0)
    chosen = jnp.zeros((EXPERTS, TOK), F32)
    weight = jnp.zeros((EXPERTS, TOK), F32)
    for k in range(8):
        hit = ids[k : k + 1, :] == row
        chosen = jnp.where(hit, 1.0, chosen)
        weight = jnp.where(hit, probs[k : k + 1, :], weight)
    earlier = jnp.where(row < col, 1.0, 0.0).astype(BF)
    rank = jnp.dot(chosen.astype(BF), earlier, preferred_element_type=F32)
    rank = jnp.where(chosen > 0.5, rank, 1000.0).T
    weight = weight.T
    rank = jnp.where(rank < limit[...].astype(F32), rank, 1000.0)
    token_id = row.astype(F32)
    for r in range(SLOTS):
        at = rank == float(r)
        meta[z, r : r + 1, :] = jnp.sum(jnp.where(at, token_id + 1000.0, 0.0), axis=0, keepdims=True) - 1000.0
        meta[z, SLOTS + r : SLOTS + r + 1, :] = jnp.sum(jnp.where(at, weight, 0.0), axis=0, keepdims=True)

    def send_meta(i, carry):
        remote(meta.at[z], meta.at[z], meta_send, meta_recv, z_peer(i)).start()
        return carry


    def ag(way, hop, c):
        block = (z + NZ - hop + 1) % NZ if way == UP else (z + hop - 1) % NZ
        return remote(
            tok.at[block, c], tok.at[block, c], ag_send.at[way, hop - 1, c], ag_recv.at[way, hop - 1, c],
            neighbour(way),
        )

    def ag_arrival(way, hop, c):
        block = (z + NZ - hop) % NZ if way == UP else (z + hop) % NZ
        return remote(
            tok.at[block, c], tok.at[block, c], ag_send.at[way, hop - 1, c], ag_recv.at[way, hop - 1, c],
            neighbour(way),
        )

    def metas():
        several = meta.at[pl.ds(0, NZ - 1)]
        return remote(several, several, meta_send, meta_recv, z_peer(1))

    def some_totals():
        some = totals.at[pl.ds(0, NX - 1)]
        return remote(some, some, tot_send, tot_recv, x_peer(1))

    def count_of(s):
        return jnp.sum(jnp.where(meta[s, 0:SLOTS, :] >= 0.0, 1.0, 0.0), axis=0, keepdims=True)

    def send_totals():
        total = jnp.zeros((1, EXPERTS), F32)
        for s in range(NZ):
            total = total + count_of(s)
        totals[x] = jnp.broadcast_to(total, (8, EXPERTS))

        def send_total(i, carry):
            remote(totals.at[x], totals.at[x], tot_send, tot_recv, x_peer(i)).start()
            return carry

        lax.fori_loop(1, NX, send_total, 0)

    def pair(k):
        return (z + NZ - k) % NZ, (z + k) % NZ

    def far_chunk(k, c):
        return c + 2 * (1 - (k % 4 + 3) // 4)

    def slot_values(first, second):
        stacked = jnp.concatenate([first, second] * PEERS, axis=0)
        s = lax.broadcasted_iota(jnp.int32, (ROWS, EXPERTS), 0)
        e = lax.broadcasted_iota(jnp.int32, (ROWS, EXPERTS), 1)
        chip = s >> 4
        expert = (chip >> 2) * (NZ * NY) + z * NY + (chip & 3)
        return jnp.sum(jnp.where(e == expert, stacked, 0.0), axis=1, keepdims=True)

    def selection(k):
        a, b = pair(k)
        source = slot_values(meta[a, 0:SLOTS, :], meta[b, 0:SLOTS, :])
        s = lax.broadcasted_iota(jnp.int32, (ROWS, 2 * TOK), 0)
        t = lax.broadcasted_iota(jnp.int32, (ROWS, 2 * TOK), 1)
        second = (s >> 3) & 1
        return (t - second * TOK).astype(F32) == source

    def exchange(src, dst, send, recv, k, c):
        def one(i, carry):
            chip, device = xy_peer(i)
            remote(src.at[k, c, rows_of(chip)], dst.at[k, c, rows_of(me)], send.at[k, c], recv.at[k, c], device).start()
            return carry

        lax.fori_loop(1, PEERS, one, 0)

    def exchanged(src, dst, send, recv, k, c):
        most = pl.ds(0, (PEERS - 1) * UNIT)
        return remote(src.at[k, c, most], dst.at[k, c, most], send.at[k, c], recv.at[k, c], x_peer(1))

    def pick_rows(k, c):
        a, b = pair(k)
        both = jnp.concatenate([tok[a, c], tok[b, far_chunk(k, c)]], axis=0)
        sbuf[k, c] = jnp.dot(mix[k], both, preferred_element_type=F32).astype(BF)
        rbuf[k, c, rows_of(me), :] = sbuf[k, c, rows_of(me), :]

    def dispatch(k, c):
        c_b = far_chunk(k, c)

        def arrive_up():
            ag_arrival(UP, k, c).wait_recv()

        def arrive_down():
            ag_arrival(DOWN, k, c_b).wait_recv()

        if c < 2:
            arrive_up()
            pl.when(k < FAR)(lambda: ag(UP, k + 1, c).start())
            arrive_down()
            pl.when(k < FAR - 1)(lambda: ag(DOWN, k + 1, c).start())
        else:
            arrive_up()
            pl.when(k < FAR - 1)(lambda: ag(UP, k + 1, c).start())
            arrive_down()
            ag(DOWN, k + 1, c).start()
        pick_rows(k, c)
        exchange(sbuf, rbuf, d_send, d_recv, k, c)

    second_half = (lax.broadcasted_iota(jnp.int32, (ROWS, 256), 0) >> 3) & 1
    second_wide = (lax.broadcasted_iota(jnp.int32, (ROWS, COLS), 0) >> 3) & 1

    def block(c):
        return slice(c * COLS, (c + 1) * COLS)

    def split_k(k):
        return (k > 0) & (k < FAR)

    def hidden(k, n):
        cols = slice(n * 256, (n + 1) * 256)

        def product(chunk, w, rows):
            return jnp.dot(rbuf[k, chunk], w[block(rows), cols], preferred_element_type=F32)

        def finish(gv, uv):
            hid[:, cols] = (gv / (1.0 + jnp.exp(-gv)) * uv).astype(BF)

        @pl.when(split_k(k))
        def _():
            finish(*(sum(product(c, w, c) for c in range(CHUNKS)) for w in (gw, uw)))

        @pl.when(jnp.logical_not(split_k(k)))
        def _():
            sums = []
            for w in (gw, uw):
                left = product(0, w, 0) + product(1, w, 1)
                right = product(0, w, 2) + product(1, w, 3)
                half = jnp.where(second_half == 0, left, right)
                swapped = jnp.where(
                    second_half == 0, pltpu.roll(half, ROWS - SLOTS, 0), pltpu.roll(half, SLOTS, 0)
                )
                sums.append(half + swapped)
            finish(*sums)

    def wait_rows(k):
        for c in range(2):
            exchanged(sbuf, rbuf, d_send, d_recv, k, c).wait_recv()

        @pl.when(split_k(k))
        def _():
            for c in range(2, CHUNKS):
                exchanged(sbuf, rbuf, d_send, d_recv, k, c).wait_recv()

    def outputs(k):
        def product(c):
            return jnp.dot(hid[...], dw[:, block(c)], preferred_element_type=F32)

        def keep(c, value):
            obuf[k, c] = value.astype(BF)
            ybuf[k, c, rows_of(me), :] = obuf[k, c, rows_of(me), :]

        @pl.when(split_k(k))
        def _():
            for c in range(CHUNKS):
                keep(c, product(c))

        @pl.when(jnp.logical_not(split_k(k)))
        def _():
            for c in range(2):
                keep(c, jnp.where(second_wide == 0, product(c), product(c + 2)))

    def weights_here():
        for i, (src, dst) in enumerate(weights):
            pltpu.make_async_copy(src, dst, w_loc.at[i]).wait()
            remote(src, theirs[i], w_send.at[i], w_recv.at[i], partner).wait_recv()

    def send_back(k):
        for c in range(2):
            exchange(obuf, ybuf, r_send, r_recv, k, c)

        @pl.when(split_k(k))
        def _():
            for c in range(2, CHUNKS):
                exchange(obuf, ybuf, r_send, r_recv, k, c)

    def weigh_all():
        some_totals().wait_recv()
        before_x = jnp.zeros((1, EXPERTS), F32)
        for s in range(NX):
            before_x = before_x + jnp.where(s < x, 1.0, 0.0) * totals[s, 0:1, :]

        def kept_weight(shard):
            offset = before_x
            for s in range(NZ):
                offset = offset + jnp.where(s < shard, 1.0, 0.0) * count_of(s)
            r = lax.broadcasted_iota(jnp.int32, (SLOTS, EXPERTS), 0).astype(F32)
            return jnp.where(offset + r < float(COL_CAP), meta[shard, SLOTS : 2 * SLOTS, :], 0.0)

        def weigh(k, carry):
            a, b = pair(k)
            w = slot_values(kept_weight(a), kept_weight(b))
            mix[k] = jnp.where(selection(k), w, 0.0).T.astype(BF)
            return carry

        lax.fori_loop(0, FAR + 1, weigh, 0)

    def step(k, carry):
        @pl.when(k == 1)
        def _():
            metas().wait_recv()
            send_totals()

        @pl.when(k <= FAR)
        def _():
            mix[k] = jnp.where(selection(k), 1.0, 0.0).astype(BF)

        for c in range(CHUNKS):
            if c < 2:
                pl.when(k <= FAR)(lambda: dispatch(k, c))
            else:
                pl.when(split_k(k))(lambda: dispatch(k, c))
            if c == 0:
                pl.when(k > 1)(lambda: hidden(k - 2, 2))
            if c == 1:
                pl.when(k > 1)(lambda: outputs(k - 2))

                @pl.when(k == FAR + 1)
                def _():
                    for early in (0, 2):
                        exchange(obuf, ybuf, r_send, r_recv, FAR - 1, early)

            if c == 2:
                pl.when(k == FAR + 1)(weigh_all)
                pl.when(k == 1)(weights_here)

                @pl.when(k < FAR + 2)
                def _():
                    wait_rows(k - 1)
                    hidden(k - 1, 0)

            if c == 3:
                pl.when(k < FAR + 2)(lambda: hidden(k - 1, 1))
        return carry

    for c in range(CHUNKS):
        own_tokens(c).wait()
    mix[0] = jnp.where(selection(0), 1.0, 0.0).astype(BF)
    for c in range(2):
        pick_rows(0, c)

    pl.semaphore_wait(barrier, NZ - 1 + PEERS - 1 + 1)
    lax.fori_loop(1, NZ, send_meta, 0)
    for c in range(CHUNKS):
        for way in range(2):
            ag(way, 1, c).start()
        if c < 2:
            exchange(sbuf, rbuf, d_send, d_recv, 0, c)
    for i, (src, dst) in enumerate(weights):
        remote(src, dst, w_send.at[i], w_recv.at[i], partner).start()

    lax.fori_loop(1, FAR + 3, step, 0)
    for c in (0, 1):
        exchange(obuf, ybuf, r_send, r_recv, FAR, c)
    for c in (1, 3):
        exchange(obuf, ybuf, r_send, r_recv, FAR - 1, c)

    def rs(way, k, c):
        return remote(
            rs_out.at[way, k - 1, c], rs_in.at[way, k - 1, c], rs_send.at[way, k - 1, c], rs_recv.at[way, k - 1, c],
            neighbour(way),
        )

    def gather_part(k, c):
        exchanged(obuf, ybuf, r_send, r_recv, k, c).wait_recv()
        part[...] = jnp.dot(mix[k], ybuf[k, c], preferred_element_type=F32)

    def mine(way):
        return slice(TOK, 2 * TOK) if way == UP else slice(0, TOK)

    def begin(c):
        gather_part(FAR - 1, c)
        later = c // 2
        rs_out[1 - later, FAR - 2, c] = part[mine(1 - later), :].astype(BF)
        rs(1 - later, FAR - 1, c).start()
        held[c] = part[mine(later), :]

    def flush(c):
        later = c // 2
        rs(later, FAR, c).wait_recv()
        rs_out[later, FAR - 2, c] = (held[c] + rs_in[later, FAR - 1, c].astype(F32)).astype(BF)
        rs(later, FAR - 1, c).start()

    def begin_far(c):
        gather_part(FAR, c)
        for way in range(2):
            rs_out[way, FAR - 1, c + 2 * way] = part[way * TOK : (way + 1) * TOK, :].astype(BF)
            rs(way, FAR, c + 2 * way).start()

    send_back(FAR - 2)
    begin(0)
    begin(2)
    begin_far(0)
    begin_far(1)
    begin(1)
    flush(0)
    flush(2)
    begin(3)
    flush(1)
    flush(3)
    for k in (0, FAR):
        for c in range(2):
            exchanged(sbuf, rbuf, d_send, d_recv, k, c).wait_send()

    def collect(i, carry):
        k = FAR - 2 - i
        send_back(k - 1)
        for c in range(CHUNKS):
            gather_part(k, c)
            for way in range(2):
                rs(way, k + 1, c).wait_recv()
                rs_out[way, k - 1, c] = (part[mine(way), :] + rs_in[way, k, c].astype(F32)).astype(BF)
                rs(way, k, c).start()
            exchanged(sbuf, rbuf, d_send, d_recv, k, c).wait_send()
            exchanged(obuf, ybuf, r_send, r_recv, k + 1, c).wait_send()
            for way in range(2):
                ag(way, k, c).wait_send()
                rs(way, k + 1, c).wait_send()
        return carry

    lax.fori_loop(0, FAR - 2, collect, 0)
    for i, (src, dst) in enumerate(weights):
        remote(src, dst, w_send.at[i], w_recv.at[i], partner).wait_send()
    metas().wait_send()
    some_totals().wait_send()
    for c in range(CHUNKS):
        exchanged(sbuf, rbuf, d_send, d_recv, FAR - 1, c).wait_send()
        for way in range(2):
            ag(way, FAR - 1, c).wait_send()
        ag(c // 2, FAR, c).wait_send()
        rs(c // 2, FAR, c).wait_send()
    for c in range(2):
        exchanged(obuf, ybuf, r_send, r_recv, FAR, c).wait_send()

    for c in range(2):
        gather_part(0, c)
        for q in range(2):
            chunk = c + 2 * q
            for way in range(2):
                rs(way, 1, chunk).wait_recv()
            out[:, block(chunk)] = (
                part[q * TOK : (q + 1) * TOK, :] + rs_in[UP, 0, chunk].astype(F32) + rs_in[DOWN, 0, chunk].astype(F32)
            ).astype(BF)

    for c in range(CHUNKS):
        exchanged(obuf, ybuf, r_send, r_recv, 1, c).wait_send()
        for way in range(2):
            rs(way, 1, c).wait_send()
    for c in range(2):
        exchanged(obuf, ybuf, r_send, r_recv, 0, c).wait_send()


def on_device(tokens, expert_ids, route_probs, shard_limit, gate_proj, up_proj, down_proj):
    dma = pltpu.SemaphoreType.DMA
    anywhere = pl.BlockSpec(memory_space=pltpu.HBM)
    near = pl.BlockSpec(memory_space=pltpu.VMEM)
    unit = (FAR + 1, CHUNKS, ROWS, COLS)
    ring = (2, FAR, CHUNKS)
    return pl.pallas_call(
        kernel,
        out_shape=jax.ShapeDtypeStruct((TOK, WIDTH), BF),
        in_specs=[anywhere, near, near, near, anywhere, anywhere, anywhere],
        out_specs=near,
        scratch_shapes=[
            pltpu.VMEM((NZ, CHUNKS, TOK, COLS), BF),
            pltpu.VMEM((NZ, 2 * SLOTS, EXPERTS), F32),
            pltpu.VMEM((NX, 8, EXPERTS), F32),
            pltpu.VMEM((WIDTH, HIDDEN), BF),
            pltpu.VMEM((WIDTH, HIDDEN), BF),
            pltpu.VMEM((HIDDEN, WIDTH), BF),
            pltpu.VMEM(unit, BF),
            pltpu.VMEM(unit, BF),
            pltpu.VMEM((ROWS, HIDDEN), BF),
            pltpu.VMEM(unit, BF),
            pltpu.VMEM(unit, BF),
            pltpu.VMEM((FAR + 1, 2 * TOK, ROWS), BF),
            pltpu.VMEM((2 * TOK, COLS), F32),
            pltpu.VMEM((CHUNKS, TOK, COLS), F32),
            pltpu.VMEM((*ring, TOK, COLS), BF),
            pltpu.VMEM((*ring, TOK, COLS), BF),
            dma((CHUNKS,)), dma((3,)), dma((3,)), dma((3,)), dma, dma, dma, dma,
            dma(ring), dma(ring),
            dma(unit[:2]), dma(unit[:2]), dma(unit[:2]), dma(unit[:2]),
            dma(ring), dma(ring),
        ],
        compiler_params=pltpu.CompilerParams(
            collective_id=0, has_side_effects=True, vmem_limit_bytes=56000000
        ),
        name="expert_layer",
    )(tokens, expert_ids.T, route_probs.T, shard_limit, gate_proj, up_proj, down_proj)


def solution(mesh):
    whole = ("dp", "expert")
    in_specs = (
        P(whole, None), P(whole, None), P(whole, None), P(whole, None),
        P(whole, None, None), P(whole, None, None), P(whole, None, None),
    )
    return jax.shard_map(
        on_device, mesh=mesh, in_specs=in_specs, out_specs=P(whole, None), check_vma=False
    )
```

```python
import jax
import jax.numpy as jnp
from jax import lax
from jax.experimental import pallas as pl
from jax.experimental.pallas import tpu as pltpu
from jax.sharding import PartitionSpec as P

MESH = pl.DeviceIdType.MESH
BF = jnp.bfloat16
F32 = jnp.float32

NX, NY, NZ = 4, 4, 8
TOK = 128
SLOTS = 8
COL_CAP = 128
WIDTH = 2048
CHUNKS = 4
COLS = WIDTH // CHUNKS
HIDDEN = 768
PEERS = NX * NY
UNIT = 2 * SLOTS
ROWS = PEERS * UNIT
EXPERTS = 128
FAR = NZ // 2
UP, DOWN = 0, 1


def kernel(
    tokens, ids, probs, limit, gate, up, down, out,
    tok, meta, totals, gw, uw, dw, sbuf, rbuf, gate_sum, up_sum, hid, obuf, ybuf, mix, part, rs_in, rs_out,
    in_sem, w_loc, w_send, w_recv, meta_send, meta_recv, tot_send, tot_recv,
    ag_send, ag_recv, d_send, d_recv, r_send, r_recv, rs_send, rs_recv,
):
    d = lax.axis_index("dp")
    c_all = lax.axis_index("expert")
    x, z = d // NZ, d % NZ
    y, core = c_all // 2, c_all % 2
    me = x * NY + y
    partner = (d, y * 2 + (1 - core))

    def z_peer(step):
        return (x * NZ + (z + step) % NZ, c_all)

    def neighbour(way):
        return z_peer(1 if way == UP else NZ - 1)

    def xy_peer(i):
        px, py = (x + i % NX) % NX, (y + i // NX) % NY
        return px * NY + py, (px * NZ + z, py * 2 + core)

    def x_peer(i):
        return (((x + i) % NX) * NZ + z, c_all)

    def rows_of(chip):
        return pl.ds(pl.multiple_of(chip * UNIT, UNIT), UNIT)

    def remote(src, dst, send, recv, device):
        return pltpu.make_async_remote_copy(
            src_ref=src, dst_ref=dst, send_sem=send, recv_sem=recv,
            device_id=device, device_id_type=MESH,
        )

    def own_tokens(c):
        return pltpu.make_async_copy(tokens.at[:, pl.ds(c * COLS, COLS)], tok.at[z, c], in_sem.at[c])

    for c in range(CHUNKS):
        own_tokens(c).start()
    wide = pl.ds(pl.multiple_of(core * (HIDDEN // 2), HIDDEN // 2), HIDDEN // 2)
    other = pl.ds(pl.multiple_of((1 - core) * (HIDDEN // 2), HIDDEN // 2), HIDDEN // 2)
    weights = (
        (gate.at[0], gw.at[:, wide]), (up.at[0], uw.at[:, wide]), (down.at[0], dw.at[wide, :]),
    )
    theirs = (gw.at[:, other], uw.at[:, other], dw.at[other, :])
    barrier = pltpu.get_barrier_semaphore()
    pl.semaphore_signal(barrier, inc=1, device_id=partner, device_id_type=MESH)

    def greet_z(i, carry):
        pl.semaphore_signal(barrier, inc=1, device_id=z_peer(i), device_id_type=MESH)
        return carry

    def greet_xy(i, carry):
        pl.semaphore_signal(barrier, inc=1, device_id=xy_peer(i)[1], device_id_type=MESH)
        return carry

    lax.fori_loop(1, NZ, greet_z, 0)
    lax.fori_loop(1, PEERS, greet_xy, 0)

    col = lax.broadcasted_iota(jnp.int32, (EXPERTS, TOK), 1)
    row = lax.broadcasted_iota(jnp.int32, (EXPERTS, TOK), 0)
    chosen = jnp.zeros((EXPERTS, TOK), F32)
    weight = jnp.zeros((EXPERTS, TOK), F32)
    for k in range(8):
        hit = ids[k : k + 1, :] == row
        chosen = jnp.where(hit, 1.0, chosen)
        weight = jnp.where(hit, probs[k : k + 1, :], weight)
    earlier = jnp.where(row < col, 1.0, 0.0).astype(BF)
    rank = jnp.dot(chosen.astype(BF), earlier, preferred_element_type=F32)
    rank = jnp.where(chosen > 0.5, rank, 1000.0).T
    weight = weight.T
    rank = jnp.where(rank < limit[...].astype(F32), rank, 1000.0)
    token_id = row.astype(F32)
    for r in range(SLOTS):
        at = rank == float(r)
        meta[z, r : r + 1, :] = jnp.sum(jnp.where(at, token_id + 1000.0, 0.0), axis=0, keepdims=True) - 1000.0
        meta[z, SLOTS + r : SLOTS + r + 1, :] = jnp.sum(jnp.where(at, weight, 0.0), axis=0, keepdims=True)

    def send_meta(i, carry):
        remote(meta.at[z], meta.at[z], meta_send, meta_recv, z_peer(i)).start()
        return carry


    def ag(way, hop, c):
        block = (z + NZ - hop + 1) % NZ if way == UP else (z + hop - 1) % NZ
        return remote(
            tok.at[block, c], tok.at[block, c], ag_send.at[way, hop - 1, c], ag_recv.at[way, hop - 1, c],
            neighbour(way),
        )

    def ag_arrival(way, hop, c):
        block = (z + NZ - hop) % NZ if way == UP else (z + hop) % NZ
        return remote(
            tok.at[block, c], tok.at[block, c], ag_send.at[way, hop - 1, c], ag_recv.at[way, hop - 1, c],
            neighbour(way),
        )

    def metas():
        several = meta.at[pl.ds(0, NZ - 1)]
        return remote(several, several, meta_send, meta_recv, z_peer(1))

    def some_totals():
        some = totals.at[pl.ds(0, NX - 1)]
        return remote(some, some, tot_send, tot_recv, x_peer(1))

    def count_of(s):
        return jnp.sum(jnp.where(meta[s, 0:SLOTS, :] >= 0.0, 1.0, 0.0), axis=0, keepdims=True)

    def send_totals():
        total = jnp.zeros((1, EXPERTS), F32)
        for s in range(NZ):
            total = total + count_of(s)
        totals[x] = jnp.broadcast_to(total, (8, EXPERTS))

        def send_total(i, carry):
            remote(totals.at[x], totals.at[x], tot_send, tot_recv, x_peer(i)).start()
            return carry

        lax.fori_loop(1, NX, send_total, 0)

    def pair(k):
        return (z + NZ - k) % NZ, (z + k) % NZ

    def far_chunk(k, c):
        return c + 2 * (1 - (k % 4 + 3) // 4)

    def slot_values(first, second):
        stacked = jnp.concatenate([first, second] * PEERS, axis=0)
        s = lax.broadcasted_iota(jnp.int32, (ROWS, EXPERTS), 0)
        e = lax.broadcasted_iota(jnp.int32, (ROWS, EXPERTS), 1)
        chip = s >> 4
        expert = (chip >> 2) * (NZ * NY) + z * NY + (chip & 3)
        return jnp.sum(jnp.where(e == expert, stacked, 0.0), axis=1, keepdims=True)

    def selection(k):
        a, b = pair(k)
        source = slot_values(meta[a, 0:SLOTS, :], meta[b, 0:SLOTS, :])
        s = lax.broadcasted_iota(jnp.int32, (ROWS, 2 * TOK), 0)
        t = lax.broadcasted_iota(jnp.int32, (ROWS, 2 * TOK), 1)
        second = (s >> 3) & 1
        return (t - second * TOK).astype(F32) == source

    def exchange(src, dst, send, recv, k, c):
        def one(i, carry):
            chip, device = xy_peer(i)
            remote(src.at[k, c, rows_of(chip)], dst.at[k, c, rows_of(me)], send.at[k, c], recv.at[k, c], device).start()
            return carry

        lax.fori_loop(1, PEERS, one, 0)

    def exchanged(src, dst, send, recv, k, c):
        most = pl.ds(0, (PEERS - 1) * UNIT)
        return remote(src.at[k, c, most], dst.at[k, c, most], send.at[k, c], recv.at[k, c], x_peer(1))

    def pick_rows(k, c):
        a, b = pair(k)
        both = jnp.concatenate([tok[a, c], tok[b, far_chunk(k, c)]], axis=0)
        sbuf[k, c] = jnp.dot(mix[k], both, preferred_element_type=F32).astype(BF)
        rbuf[k, c, rows_of(me), :] = sbuf[k, c, rows_of(me), :]

    def dispatch(k, c):
        c_b = far_chunk(k, c)

        def arrive_up():
            ag_arrival(UP, k, c).wait_recv()

        def arrive_down():
            ag_arrival(DOWN, k, c_b).wait_recv()

        if c < 2:
            arrive_up()
            pl.when(k < FAR)(lambda: ag(UP, k + 1, c).start())
            arrive_down()
            pl.when(k < FAR - 1)(lambda: ag(DOWN, k + 1, c).start())
        else:
            arrive_up()
            pl.when(k < FAR - 1)(lambda: ag(UP, k + 1, c).start())
            arrive_down()
            ag(DOWN, k + 1, c).start()
        pick_rows(k, c)
        exchange(sbuf, rbuf, d_send, d_recv, k, c)

    second_half = (lax.broadcasted_iota(jnp.int32, (ROWS, 256), 0) >> 3) & 1
    second_wide = (lax.broadcasted_iota(jnp.int32, (ROWS, COLS), 0) >> 3) & 1

    def block(c):
        return slice(c * COLS, (c + 1) * COLS)

    def split_k(k):
        return (k > 0) & (k < FAR)

    def arrived(k, c):
        exchanged(sbuf, rbuf, d_send, d_recv, k, c).wait_recv()

    def add_chunk(k, c, spread, fresh):
        arrived(k, c)
        for total, w in ((gate_sum, gw), (up_sum, uw)):
            for n in range(0, HIDDEN, 256):
                cols = slice(n, n + 256)
                value = jnp.dot(rbuf[k, c], w[block(c), cols], preferred_element_type=F32)
                if spread:
                    right = jnp.dot(rbuf[k, c], w[block(c + 2), cols], preferred_element_type=F32)
                    value = jnp.where(second_half == 0, value, right)
                total[:, cols] = value if fresh else total[:, cols] + value

    def activate(spread):
        for n in range(0, HIDDEN, 256):
            cols = slice(n, n + 256)
            values = []
            for total in (gate_sum, up_sum):
                value = total[:, cols]
                if spread:
                    value = value + jnp.where(
                        second_half == 0, pltpu.roll(value, ROWS - SLOTS, 0), pltpu.roll(value, SLOTS, 0)
                    )
                values.append(value)
            gv, uv = values
            hid[:, cols] = (gv / (1.0 + jnp.exp(-gv)) * uv).astype(BF)

    def outputs(k):
        for c in range(2):
            left, right = (
                jnp.dot(hid[...], dw[:, block(chunk)], preferred_element_type=F32) for chunk in (c, c + 2)
            )
            obuf[k, c] = jnp.where(second_wide == 0, left, right).astype(BF)
            ybuf[k, c, rows_of(me), :] = obuf[k, c, rows_of(me), :]

            @pl.when(split_k(k))
            def _():
                obuf[k, c + 2] = jnp.where(second_wide == 0, right, left).astype(BF)
                ybuf[k, c + 2, rows_of(me), :] = obuf[k, c + 2, rows_of(me), :]

    def weights_here():
        for i, (src, dst) in enumerate(weights):
            pltpu.make_async_copy(src, dst, w_loc.at[i]).wait()
            remote(src, theirs[i], w_send.at[i], w_recv.at[i], partner).wait_recv()

    def send_back(k):
        for c in range(2):
            exchange(obuf, ybuf, r_send, r_recv, k, c)

        @pl.when(split_k(k))
        def _():
            for c in range(2, CHUNKS):
                exchange(obuf, ybuf, r_send, r_recv, k, c)

    def weigh_all():
        some_totals().wait_recv()
        before_x = jnp.zeros((1, EXPERTS), F32)
        for s in range(NX):
            before_x = before_x + jnp.where(s < x, 1.0, 0.0) * totals[s, 0:1, :]

        def kept_weight(shard):
            offset = before_x
            for s in range(NZ):
                offset = offset + jnp.where(s < shard, 1.0, 0.0) * count_of(s)
            r = lax.broadcasted_iota(jnp.int32, (SLOTS, EXPERTS), 0).astype(F32)
            return jnp.where(offset + r < float(COL_CAP), meta[shard, SLOTS : 2 * SLOTS, :], 0.0)

        def weigh(k, carry):
            a, b = pair(k)
            w = slot_values(kept_weight(a), kept_weight(b))
            mix[k] = jnp.where(selection(k), w, 0.0).T.astype(BF)
            return carry

        lax.fori_loop(0, FAR + 1, weigh, 0)

    def step(k, carry):
        @pl.when(k == 1)
        def _():
            metas().wait_recv()
            send_totals()

        @pl.when(k <= FAR)
        def _():
            mix[k] = jnp.where(selection(k), 1.0, 0.0).astype(BF)

        for c in range(CHUNKS):
            if c < 2:
                pl.when(k <= FAR)(lambda: dispatch(k, c))
            else:
                pl.when(split_k(k))(lambda: dispatch(k, c))
            if c < 2:
                pl.when((k > 1) & (k <= FAR))(lambda: add_chunk(k - 1, c + 1, False, False))
            if c == 2:
                @pl.when(k == 1)
                def _():
                    weights_here()
                    add_chunk(0, 0, True, True)
                    add_chunk(0, 1, True, False)
                    activate(True)

                @pl.when((k > 1) & (k <= FAR))
                def _():
                    add_chunk(k - 1, 3, False, False)
                    activate(False)

                @pl.when(k == FAR + 1)
                def _():
                    add_chunk(FAR, 1, True, False)
                    activate(True)

            if c == 3:
                outputs(k - 1)
                pl.when(k < FAR)(lambda: add_chunk(k, 0, False, True))

                @pl.when(k == FAR)
                def _():
                    for early in range(2):
                        exchange(obuf, ybuf, r_send, r_recv, FAR - 1, early)
                    weigh_all()
                    add_chunk(FAR, 0, True, True)

        return carry

    for c in range(CHUNKS):
        own_tokens(c).wait()
    for i, (src, dst) in enumerate(weights):
        pltpu.make_async_copy(src, dst, w_loc.at[i]).start()
    mix[0] = jnp.where(selection(0), 1.0, 0.0).astype(BF)
    for c in range(2):
        pick_rows(0, c)

    pl.semaphore_wait(barrier, NZ - 1 + PEERS - 1 + 1)
    lax.fori_loop(1, NZ, send_meta, 0)
    for c in range(CHUNKS):
        for way in range(2):
            ag(way, 1, c).start()
        if c < 2:
            exchange(sbuf, rbuf, d_send, d_recv, 0, c)
    for i, (src, dst) in enumerate(weights):
        remote(src, dst, w_send.at[i], w_recv.at[i], partner).start()

    lax.fori_loop(1, FAR + 2, step, 0)
    for c in (0, 1):
        exchange(obuf, ybuf, r_send, r_recv, FAR, c)
    for c in (2, 3):
        exchange(obuf, ybuf, r_send, r_recv, FAR - 1, c)

    def rs(way, k, c):
        return remote(
            rs_out.at[way, k - 1, c], rs_in.at[way, k - 1, c], rs_send.at[way, k - 1, c], rs_recv.at[way, k - 1, c],
            neighbour(way),
        )

    def gather_part(k, c):
        exchanged(obuf, ybuf, r_send, r_recv, k, c).wait_recv()
        part[...] = jnp.dot(mix[k], ybuf[k, c], preferred_element_type=F32)

    def mine(way):
        return slice(TOK, 2 * TOK) if way == UP else slice(0, TOK)

    def chunk_of(way, c):
        return (c + 2) % CHUNKS if way == UP else c

    def pass_on(way, k, c):
        chunk = chunk_of(way, c)
        rs(way, k + 1, chunk).wait_recv()
        rs_out[way, k - 1, chunk] = (part[mine(way), :] + rs_in[way, k, chunk].astype(F32)).astype(BF)
        rs(way, k, chunk).start()

    def begin(c):
        gather_part(FAR - 1, c)
        for way in range(2):
            if c < 2:
                rs_out[way, FAR - 2, chunk_of(way, c)] = part[mine(way), :].astype(BF)
                rs(way, FAR - 1, chunk_of(way, c)).start()
            else:
                pass_on(way, FAR - 1, c)

    def begin_far(c):
        gather_part(FAR, c)
        for way in range(2):
            rs_out[way, FAR - 1, c + 2 * way] = part[way * TOK : (way + 1) * TOK, :].astype(BF)
            rs(way, FAR, c + 2 * way).start()

    send_back(FAR - 2)
    begin(0)
    begin(1)
    begin_far(0)
    begin_far(1)
    begin(2)
    begin(3)
    for k in (0, FAR):
        for c in range(2):
            exchanged(sbuf, rbuf, d_send, d_recv, k, c).wait_send()

    def collect(i, carry):
        k = FAR - 2 - i
        send_back(k - 1)
        for c in range(CHUNKS):
            gather_part(k, c)
            for way in range(2):
                pass_on(way, k, c)
            exchanged(sbuf, rbuf, d_send, d_recv, k, c).wait_send()
            exchanged(obuf, ybuf, r_send, r_recv, k + 1, c).wait_send()
            for way in range(2):
                ag(way, k, c).wait_send()
                rs(way, k + 1, c).wait_send()
        return carry

    lax.fori_loop(0, FAR - 2, collect, 0)
    for i, (src, dst) in enumerate(weights):
        remote(src, dst, w_send.at[i], w_recv.at[i], partner).wait_send()
    metas().wait_send()
    some_totals().wait_send()
    for c in range(CHUNKS):
        exchanged(sbuf, rbuf, d_send, d_recv, FAR - 1, c).wait_send()
        for way in range(2):
            ag(way, FAR - 1, c).wait_send()
        ag(c // 2, FAR, c).wait_send()
        rs(c // 2, FAR, c).wait_send()
    for c in range(2):
        exchanged(obuf, ybuf, r_send, r_recv, FAR, c).wait_send()

    for c in range(2):
        gather_part(0, c)
        for q in range(2):
            chunk = c + 2 * q
            for way in range(2):
                rs(way, 1, chunk).wait_recv()
            out[:, block(chunk)] = (
                part[q * TOK : (q + 1) * TOK, :] + rs_in[UP, 0, chunk].astype(F32) + rs_in[DOWN, 0, chunk].astype(F32)
            ).astype(BF)

    for c in range(CHUNKS):
        exchanged(obuf, ybuf, r_send, r_recv, 1, c).wait_send()
        for way in range(2):
            rs(way, 1, c).wait_send()
    for c in range(2):
        exchanged(obuf, ybuf, r_send, r_recv, 0, c).wait_send()


def on_device(tokens, expert_ids, route_probs, shard_limit, gate_proj, up_proj, down_proj):
    dma = pltpu.SemaphoreType.DMA
    anywhere = pl.BlockSpec(memory_space=pltpu.HBM)
    near = pl.BlockSpec(memory_space=pltpu.VMEM)
    unit = (FAR + 1, CHUNKS, ROWS, COLS)
    ring = (2, FAR, CHUNKS)
    return pl.pallas_call(
        kernel,
        out_shape=jax.ShapeDtypeStruct((TOK, WIDTH), BF),
        in_specs=[anywhere, near, near, near, anywhere, anywhere, anywhere],
        out_specs=near,
        scratch_shapes=[
            pltpu.VMEM((NZ, CHUNKS, TOK, COLS), BF),
            pltpu.VMEM((NZ, 2 * SLOTS, EXPERTS), F32),
            pltpu.VMEM((NX, 8, EXPERTS), F32),
            pltpu.VMEM((WIDTH, HIDDEN), BF),
            pltpu.VMEM((WIDTH, HIDDEN), BF),
            pltpu.VMEM((HIDDEN, WIDTH), BF),
            pltpu.VMEM(unit, BF),
            pltpu.VMEM(unit, BF),
            pltpu.VMEM((ROWS, HIDDEN), F32),
            pltpu.VMEM((ROWS, HIDDEN), F32),
            pltpu.VMEM((ROWS, HIDDEN), BF),
            pltpu.VMEM(unit, BF),
            pltpu.VMEM(unit, BF),
            pltpu.VMEM((FAR + 1, 2 * TOK, ROWS), BF),
            pltpu.VMEM((2 * TOK, COLS), F32),
            pltpu.VMEM((*ring, TOK, COLS), BF),
            pltpu.VMEM((*ring, TOK, COLS), BF),
            dma((CHUNKS,)), dma((3,)), dma((3,)), dma((3,)), dma, dma, dma, dma,
            dma(ring), dma(ring),
            dma(unit[:2]), dma(unit[:2]), dma(unit[:2]), dma(unit[:2]),
            dma(ring), dma(ring),
        ],
        compiler_params=pltpu.CompilerParams(
            collective_id=0, has_side_effects=True, vmem_limit_bytes=56000000
        ),
        name="expert_layer",
    )(tokens, expert_ids.T, route_probs.T, shard_limit, gate_proj, up_proj, down_proj)


def solution(mesh):
    whole = ("dp", "expert")
    in_specs = (
        P(whole, None), P(whole, None), P(whole, None), P(whole, None),
        P(whole, None, None), P(whole, None, None), P(whole, None, None),
    )
    return jax.shard_map(
        on_device, mesh=mesh, in_specs=in_specs, out_specs=P(whole, None), check_vma=False
    )
```

```python
import jax
import jax.numpy as jnp
from jax import lax
from jax.experimental import pallas as pl
from jax.experimental.pallas import tpu as pltpu
from jax.sharding import PartitionSpec as P

MESH = pl.DeviceIdType.MESH
BF = jnp.bfloat16
F32 = jnp.float32

NX, NY, NZ = 4, 4, 8
TOK = 128
SLOTS = 8
COL_CAP = 128
WIDTH = 2048
CHUNKS = 4
COLS = WIDTH // CHUNKS
HIDDEN = 768
PEERS = NX * NY
UNIT = 2 * SLOTS
ROWS = PEERS * UNIT
EXPERTS = 128
FAR = NZ // 2
UP, DOWN = 0, 1


def mod(a, n):
    return a % n if isinstance(a, int) else lax.rem(a, n)


def div(a, n):
    return a // n if isinstance(a, int) else lax.div(a, n)


def kernel(
    tokens, route, probs, gate, up, down, out,
    tok, meta, totals, gw, uw, dw, sbuf, rbuf, gate_sum, up_sum, hid, obuf, ybuf, mix, part, rs_in, rs_out,
    in_sem, w_loc, w_send, w_recv, meta_send, meta_recv, tot_send, tot_recv,
    ag_send, ag_recv, d_send, d_recv, r_send, r_recv, rs_send, rs_recv,
):
    d = lax.axis_index("dp")
    c_all = lax.axis_index("expert")
    x, z = div(d, NZ), mod(d, NZ)
    y, core = div(c_all, 2), mod(c_all, 2)
    me = x * NY + y
    partner = (d, y * 2 + (1 - core))

    def z_peer(step):
        return (x * NZ + mod(z + step, NZ), c_all)

    def neighbour(way):
        return z_peer(1 if way == UP else NZ - 1)

    def xy_peer(i):
        px, py = mod(x + mod(i, NX), NX), mod(y + div(i, NX), NY)
        return px * NY + py, (px * NZ + z, py * 2 + core)

    def x_peer(i):
        return (mod(x + i, NX) * NZ + z, c_all)

    def rows_of(chip):
        return pl.ds(pl.multiple_of(chip * UNIT, UNIT), UNIT)

    def remote(src, dst, send, recv, device):
        return pltpu.make_async_remote_copy(
            src_ref=src, dst_ref=dst, send_sem=send, recv_sem=recv,
            device_id=device, device_id_type=MESH,
        )

    def own_tokens(c):
        return pltpu.make_async_copy(tokens.at[:, pl.ds(c * COLS, COLS)], tok.at[z, c], in_sem)

    for c in range(CHUNKS):
        own_tokens(c).start()
    wide = pl.ds(pl.multiple_of(core * (HIDDEN // 2), HIDDEN // 2), HIDDEN // 2)
    other = pl.ds(pl.multiple_of((1 - core) * (HIDDEN // 2), HIDDEN // 2), HIDDEN // 2)
    weights = (
        (gate.at[0], gw.at[:, wide]), (up.at[0], uw.at[:, wide]), (down.at[0], dw.at[wide, :]),
    )
    theirs = (gw.at[:, other], uw.at[:, other], dw.at[other, :])
    barrier = pltpu.get_barrier_semaphore()
    pl.semaphore_signal(barrier, inc=1, device_id=partner, device_id_type=MESH)

    def greet_z(i, carry):
        pl.semaphore_signal(barrier, inc=1, device_id=z_peer(i), device_id_type=MESH)
        return carry

    def greet_xy(i, carry):
        pl.semaphore_signal(barrier, inc=1, device_id=xy_peer(i)[1], device_id_type=MESH)
        return carry

    lax.fori_loop(1, NZ, greet_z, 0)
    lax.fori_loop(1, PEERS, greet_xy, 0)

    col = lax.broadcasted_iota(jnp.int32, (EXPERTS, TOK), 1)
    row = lax.broadcasted_iota(jnp.int32, (EXPERTS, TOK), 0)
    chosen = jnp.zeros((EXPERTS, TOK), F32)
    weight = jnp.zeros((EXPERTS, TOK), F32)
    for k in range(8):
        hit = (route[k : k + 1, :] >> 4) == row
        chosen = jnp.where(hit, 1.0, chosen)
        weight = jnp.where(hit, probs[k : k + 1, :], weight)
    earlier = jnp.where(row < col, 1.0, 0.0).astype(BF)
    rank = jnp.dot(chosen.astype(BF), earlier, preferred_element_type=F32)
    rank = jnp.where(chosen > 0.5, rank, 1000.0).T
    weight = weight.T
    rank = jnp.where(rank < (route[0:1, :] & 15).astype(F32), rank, 1000.0)
    token_id = row.astype(F32)
    for r in range(SLOTS):
        at = rank == float(r)
        meta[z, r : r + 1, :] = jnp.sum(jnp.where(at, token_id + 1000.0, 0.0), axis=0, keepdims=True) - 1000.0
        meta[z, SLOTS + r : SLOTS + r + 1, :] = jnp.sum(jnp.where(at, weight, 0.0), axis=0, keepdims=True)

    def send_meta(i, carry):
        remote(meta.at[z], meta.at[z], meta_send, meta_recv, z_peer(i)).start()
        return carry


    def unit_of(hop, c):
        return c - 2 * div(hop, FAR) * (c // 2)

    def ag(way, hop, c):
        block = mod(z + NZ - hop + 1, NZ) if way == UP else mod(z + hop - 1, NZ)
        return remote(
            tok.at[block, c], tok.at[block, c], ag_send, ag_recv.at[hop - 1, unit_of(hop, c)],
            neighbour(way),
        )

    def ag_arrived(hop, c):
        two = tok.at[pl.ds(0, 2), c]
        remote(two, two, ag_send, ag_recv.at[hop - 1, c], z_peer(1)).wait_recv()

    def metas():
        several = meta.at[pl.ds(0, NZ - 1)]
        return remote(several, several, meta_send, meta_recv, z_peer(1))

    def some_totals():
        some = totals.at[pl.ds(0, NX - 1)]
        return remote(some, some, tot_send, tot_recv, x_peer(1))

    def count_of(s):
        return jnp.sum(jnp.where(meta[s, 0:SLOTS, :] >= 0.0, 1.0, 0.0), axis=0, keepdims=True)

    def send_totals():
        total = jnp.zeros((1, EXPERTS), F32)
        for s in range(NZ):
            total = total + count_of(s)
        totals[x] = jnp.broadcast_to(total, (8, EXPERTS))

        def send_total(i, carry):
            remote(totals.at[x], totals.at[x], tot_send, tot_recv, x_peer(i)).start()
            return carry

        lax.fori_loop(1, NX, send_total, 0)

    def pair(k):
        return mod(z + NZ - k, NZ), mod(z + k, NZ)

    def far_chunk(k, c):
        return c + 2 * (1 - div(mod(k, 4) + 3, 4))

    def slot_values(first, second):
        stacked = jnp.concatenate([first, second] * PEERS, axis=0)
        s = lax.broadcasted_iota(jnp.int32, (ROWS, EXPERTS), 0)
        e = lax.broadcasted_iota(jnp.int32, (ROWS, EXPERTS), 1)
        chip = s >> 4
        expert = (chip >> 2) * (NZ * NY) + z * NY + (chip & 3)
        return jnp.sum(jnp.where(e == expert, stacked, 0.0), axis=1, keepdims=True)

    def selection(k):
        a, b = pair(k)
        source = slot_values(meta[a, 0:SLOTS, :], meta[b, 0:SLOTS, :])
        s = lax.broadcasted_iota(jnp.int32, (ROWS, 2 * TOK), 0)
        t = lax.broadcasted_iota(jnp.int32, (ROWS, 2 * TOK), 1)
        second = (s >> 3) & 1
        return (t - second * TOK).astype(F32) == source

    def exchange(src, dst, send, recv, k, c):
        def one(i, carry):
            chip, device = xy_peer(PEERS - i)
            remote(src.at[k, c, rows_of(chip)], dst.at[k, c, rows_of(me)], send, recv.at[k, c], device).start()
            return carry

        lax.fori_loop(1, PEERS, one, 0)

    def exchanged(src, dst, send, recv, k, c):
        most = pl.ds(0, (PEERS - 1) * UNIT)
        return remote(src.at[k, c, most], dst.at[k, c, most], send, recv.at[k, c], x_peer(1))

    def pick_rows(k, c):
        a, b = pair(k)
        both = jnp.concatenate([tok[a, c], tok[b, far_chunk(k, c)]], axis=0)
        sbuf[k, c] = jnp.dot(mix[k], both, preferred_element_type=F32).astype(BF)
        rbuf[k, c, rows_of(me), :] = sbuf[k, c, rows_of(me), :]

    def dispatch(k, c):
        ag_arrived(k, c)
        if c < 2:
            pl.when(k < FAR)(lambda: ag(UP, k + 1, c).start())
            pl.when(k < FAR - 1)(lambda: ag(DOWN, k + 1, c).start())
        else:
            pl.when(k < FAR - 1)(lambda: ag(UP, k + 1, c).start())
            ag(DOWN, k + 1, c).start()
        pick_rows(k, c)
        exchange(sbuf, rbuf, d_send, d_recv, k, c)

    second_half = (lax.broadcasted_iota(jnp.int32, (ROWS, 256), 0) >> 3) & 1
    second_wide = (lax.broadcasted_iota(jnp.int32, (ROWS, COLS), 0) >> 3) & 1

    def block(c):
        return slice(c * COLS, (c + 1) * COLS)

    def split_k(k):
        return (k > 0) & (k < FAR)

    def arrived(k, c):
        exchanged(sbuf, rbuf, d_send, d_recv, k, c).wait_recv()

    def add_chunk(k, c, spread, fresh):
        arrived(k, c)
        for total, w in ((gate_sum, gw), (up_sum, uw)):
            for n in range(0, HIDDEN, 256):
                cols = slice(n, n + 256)
                value = jnp.dot(rbuf[k, c], w[block(c), cols], preferred_element_type=F32)
                if spread:
                    right = jnp.dot(rbuf[k, c], w[block(c + 2), cols], preferred_element_type=F32)
                    value = jnp.where(second_half == 0, value, right)
                total[:, cols] = value if fresh else total[:, cols] + value

    def activate(spread):
        for n in range(0, HIDDEN, 256):
            cols = slice(n, n + 256)
            values = []
            for total in (gate_sum, up_sum):
                value = total[:, cols]
                if spread:
                    value = value + jnp.where(
                        second_half == 0, pltpu.roll(value, ROWS - SLOTS, 0), pltpu.roll(value, SLOTS, 0)
                    )
                values.append(value)
            gv, uv = values
            hid[:, cols] = (gv / (1.0 + jnp.exp(-gv)) * uv).astype(BF)

    def outputs(k):
        for c in range(2):
            left, right = (
                jnp.dot(hid[...], dw[:, block(chunk)], preferred_element_type=F32) for chunk in (c, c + 2)
            )
            obuf[k, c] = jnp.where(second_wide == 0, left, right).astype(BF)
            ybuf[k, c, rows_of(me), :] = obuf[k, c, rows_of(me), :]

            @pl.when(split_k(k))
            def _():
                obuf[k, c + 2] = jnp.where(second_wide == 0, right, left).astype(BF)
                ybuf[k, c + 2, rows_of(me), :] = obuf[k, c + 2, rows_of(me), :]

    def weights_here():
        for i, (src, dst) in enumerate(weights):
            pltpu.make_async_copy(src, dst, w_loc.at[i]).wait()
            remote(src, theirs[i], w_send.at[i], w_recv.at[i], partner).wait_recv()

    def weigh_all():
        some_totals().wait_recv()
        before_x = jnp.zeros((1, EXPERTS), F32)
        for s in range(NX):
            before_x = before_x + jnp.where(s < x, 1.0, 0.0) * totals[s, 0:1, :]

        def kept_weight(shard):
            offset = before_x
            for s in range(NZ):
                offset = offset + jnp.where(s < shard, 1.0, 0.0) * count_of(s)
            r = lax.broadcasted_iota(jnp.int32, (SLOTS, EXPERTS), 0).astype(F32)
            return jnp.where(offset + r < float(COL_CAP), meta[shard, SLOTS : 2 * SLOTS, :], 0.0)

        def weigh(k, carry):
            a, b = pair(k)
            w = slot_values(kept_weight(a), kept_weight(b))
            mix[k] = jnp.where(selection(k), w, 0.0).T.astype(BF)
            return carry

        lax.fori_loop(0, FAR + 1, weigh, 0)

    def step(k, carry):
        @pl.when(k == 1)
        def _():
            metas().wait_recv()
            send_totals()

        @pl.when(k <= FAR)
        def _():
            mix[k] = jnp.where(selection(k), 1.0, 0.0).astype(BF)

        for c in range(CHUNKS):
            if c < 2:
                pl.when(k <= FAR)(lambda: dispatch(k, c))
            else:
                pl.when(split_k(k))(lambda: dispatch(k, c))
            if c < 2:
                pl.when((k > 1) & (k <= FAR))(lambda: add_chunk(k - 1, c + 1, False, False))
            if c == 2:
                @pl.when(k == 1)
                def _():
                    weights_here()
                    add_chunk(0, 0, True, True)
                    add_chunk(0, 1, True, False)
                    activate(True)

                @pl.when((k > 1) & (k <= FAR))
                def _():
                    add_chunk(k - 1, 3, False, False)
                    activate(False)

                @pl.when(k == FAR + 1)
                def _():
                    add_chunk(FAR, 1, True, False)
                    activate(True)

            if c == 3:
                outputs(k - 1)
                pl.when(k < FAR)(lambda: add_chunk(k, 0, False, True))

                @pl.when(k == FAR)
                def _():
                    for early in range(2):
                        exchange(obuf, ybuf, r_send, r_recv, FAR - 1, early)
                    weigh_all()
                    add_chunk(FAR, 0, True, True)

        return carry

    pltpu.make_async_copy(tok.at[z], tok.at[z], in_sem).wait()
    for i, (src, dst) in enumerate(weights):
        pltpu.make_async_copy(src, dst, w_loc.at[i]).start()
    mix[0] = jnp.where(selection(0), 1.0, 0.0).astype(BF)
    for c in range(2):
        pick_rows(0, c)

    pl.semaphore_wait(barrier, NZ - 1 + PEERS - 1 + 1)
    lax.fori_loop(1, NZ, send_meta, 0)
    for c in range(CHUNKS):
        for way in range(2):
            ag(way, 1, c).start()
        if c < 2:
            exchange(sbuf, rbuf, d_send, d_recv, 0, c)
    for i, (src, dst) in enumerate(weights):
        remote(src, dst, w_send.at[i], w_recv.at[i], partner).start()

    lax.fori_loop(1, FAR + 2, step, 0)
    for c in (0, 1):
        exchange(obuf, ybuf, r_send, r_recv, FAR, c)
    def rs(way, k, c):
        unit = c if way == DOWN else mod(c + 2, CHUNKS)
        return remote(
            rs_out.at[way, k - 1, c], rs_in.at[way, k - 1, c], rs_send, rs_recv.at[k - 1, unit], neighbour(way)
        )

    def rs_arrived(k, unit):
        two = rs_in.at[pl.ds(0, 2), k - 1, unit]
        remote(two, two, rs_send, rs_recv.at[k - 1, unit], z_peer(1)).wait_recv()

    def gather_part(k, c):
        exchanged(obuf, ybuf, r_send, r_recv, k, c).wait_recv()
        part[...] = jnp.dot(mix[k], ybuf[k, c], preferred_element_type=F32)

    def mine(way):
        return slice(TOK, 2 * TOK) if way == UP else slice(0, TOK)

    def chunk_of(way, c):
        return (c + 2) % CHUNKS if way == UP else c

    def pass_on(way, k, c):
        chunk = chunk_of(way, c)
        rs_out[way, k - 1, chunk] = (part[mine(way), :] + rs_in[way, k, chunk].astype(F32)).astype(BF)
        rs(way, k, chunk).start()

    def begin(c):
        gather_part(FAR - 1, c)
        if c >= 2:
            rs_arrived(FAR, c)
        for way in range(2):
            if c < 2:
                rs_out[way, FAR - 2, chunk_of(way, c)] = part[mine(way), :].astype(BF)
                rs(way, FAR - 1, chunk_of(way, c)).start()
            else:
                pass_on(way, FAR - 1, c)

    def begin_far(c):
        gather_part(FAR, c)
        for way in range(2):
            rs_out[way, FAR - 1, c + 2 * way] = part[way * TOK : (way + 1) * TOK, :].astype(BF)
            rs(way, FAR, c + 2 * way).start()

    begin(0)
    begin(1)
    for c in (2, 3):
        exchange(obuf, ybuf, r_send, r_recv, FAR - 1, c)
    begin_far(0)
    exchange(obuf, ybuf, r_send, r_recv, FAR - 2, 0)
    begin_far(1)
    exchange(obuf, ybuf, r_send, r_recv, FAR - 2, 1)
    for c in (2, 3):
        begin(c)
        exchange(obuf, ybuf, r_send, r_recv, FAR - 2, c)

    def collect(i, carry):
        k = FAR - 2 - i
        for c in range(CHUNKS):
            gather_part(k, c)
            rs_arrived(k + 1, c)
            for way in range(2):
                pass_on(way, k, c)
            if c < 2:
                exchange(obuf, ybuf, r_send, r_recv, k - 1, c)
            else:
                pl.when(k > 1)(lambda: exchange(obuf, ybuf, r_send, r_recv, k - 1, c))
        return carry

    lax.fori_loop(0, FAR - 2, collect, 0)
    for i, (src, dst) in enumerate(weights):
        remote(src, dst, w_send.at[i], w_recv.at[i], partner).wait_send()
    metas().wait_send()
    some_totals().wait_send()
    blocks = tok.at[pl.ds(0, NZ - 1)]
    remote(blocks, blocks, ag_send, ag_recv.at[0, 0], z_peer(1)).wait_send()
    rows = sbuf.at[pl.ds(0, FAR), :, pl.ds(0, (PEERS - 1) * UNIT)]
    remote(rows, rows, d_send, d_recv.at[0, 0], x_peer(1)).wait_send()

    for c in range(2):
        gather_part(0, c)
        for q in range(2):
            rs_arrived(1, c + 2 * q)
        for q in range(2):
            chunk = c + 2 * q
            out[:, block(chunk)] = (
                part[q * TOK : (q + 1) * TOK, :] + rs_in[UP, 0, chunk].astype(F32) + rs_in[DOWN, 0, chunk].astype(F32)
            ).astype(BF)

    remote(rows, rows, r_send, r_recv.at[0, 0], x_peer(1)).wait_send()
    sums = rs_out.at[:, :, :, pl.ds(0, TOK * (NZ - 1) // NZ)]
    remote(sums, sums, rs_send, rs_recv.at[0, 0], z_peer(1)).wait_send()


def on_device(tokens, expert_ids, route_probs, shard_limit, gate_proj, up_proj, down_proj):
    dma = pltpu.SemaphoreType.DMA
    route = expert_ids.T * 16 + shard_limit
    anywhere = pl.BlockSpec(memory_space=pltpu.HBM)
    near = pl.BlockSpec(memory_space=pltpu.VMEM)
    unit = (FAR + 1, CHUNKS, ROWS, COLS)
    ring = (2, FAR, CHUNKS)
    return pl.pallas_call(
        kernel,
        out_shape=jax.ShapeDtypeStruct((TOK, WIDTH), BF),
        in_specs=[anywhere, near, near, anywhere, anywhere, anywhere],
        out_specs=near,
        scratch_shapes=[
            pltpu.VMEM((NZ, CHUNKS, TOK, COLS), BF),
            pltpu.VMEM((NZ, 2 * SLOTS, EXPERTS), F32),
            pltpu.VMEM((NX, 8, EXPERTS), F32),
            pltpu.VMEM((WIDTH, HIDDEN), BF),
            pltpu.VMEM((WIDTH, HIDDEN), BF),
            pltpu.VMEM((HIDDEN, WIDTH), BF),
            pltpu.VMEM(unit, BF),
            pltpu.VMEM(unit, BF),
            pltpu.VMEM((ROWS, HIDDEN), F32),
            pltpu.VMEM((ROWS, HIDDEN), F32),
            pltpu.VMEM((ROWS, HIDDEN), BF),
            pltpu.VMEM(unit, BF),
            pltpu.VMEM(unit, BF),
            pltpu.VMEM((FAR + 1, 2 * TOK, ROWS), BF),
            pltpu.VMEM((2 * TOK, COLS), F32),
            pltpu.VMEM((*ring, TOK, COLS), BF),
            pltpu.VMEM((*ring, TOK, COLS), BF),
            dma, dma((3,)), dma((3,)), dma((3,)), dma, dma, dma, dma,
            dma, dma(ring[1:]), dma, dma(unit[:2]), dma, dma(unit[:2]), dma, dma(ring[1:]),
        ],
        compiler_params=pltpu.CompilerParams(
            collective_id=0, has_side_effects=True, vmem_limit_bytes=56000000
        ),
        name="expert_layer",
    )(tokens, route, route_probs.T, gate_proj, up_proj, down_proj)


def solution(mesh):
    whole = ("dp", "expert")
    in_specs = (
        P(whole, None), P(whole, None), P(whole, None), P(whole, None),
        P(whole, None, None), P(whole, None, None), P(whole, None, None),
    )
    return jax.shard_map(
        on_device, mesh=mesh, in_specs=in_specs, out_specs=P(whole, None), check_vma=False
    )
```

```python
import jax
import jax.numpy as jnp
from jax import lax
from jax.experimental import pallas as pl
from jax.experimental.pallas import tpu as pltpu
from jax.sharding import PartitionSpec as P

MESH = pl.DeviceIdType.MESH
BF = jnp.bfloat16
F32 = jnp.float32

NX, NY, NZ = 4, 4, 8
TOK = 128
SLOTS = 8
COL_CAP = 128
WIDTH = 2048
CHUNKS = 4
COLS = WIDTH // CHUNKS
HIDDEN = 768
PEERS = NX * NY
UNIT = 2 * SLOTS
ROWS = PEERS * UNIT
EXPERTS = 128
FAR = NZ // 2
UP, DOWN = 0, 1


def mod(a, n):
    return a % n if isinstance(a, int) else lax.rem(a, n)


def div(a, n):
    return a // n if isinstance(a, int) else lax.div(a, n)


def kernel(
    tokens, ids_in, probs_in, limit_in, gate, up, down, out,
    ids, probs, limit, tok, meta, totals, gw, uw, dw, sbuf, rbuf, gate_sum, up_sum, hid, obuf, ybuf, mix, part, rs_in, rs_out,
    route_sem, in_sem, w_loc, w_send, w_recv, meta_send, meta_recv, tot_send, tot_recv,
    ag_send, ag_recv, d_send, d_recv, r_send, r_recv, rs_send, rs_recv,
):
    d = lax.axis_index("dp")
    c_all = lax.axis_index("expert")
    x, z = div(d, NZ), mod(d, NZ)
    y, core = div(c_all, 2), mod(c_all, 2)
    me = x * NY + y
    partner = (d, y * 2 + (1 - core))

    def z_peer(step):
        return (x * NZ + mod(z + step, NZ), c_all)

    def neighbour(way):
        return z_peer(1 if way == UP else NZ - 1)

    def xy_peer(i):
        px, py = mod(x + mod(i, NX), NX), mod(y + div(i, NX), NY)
        return px * NY + py, (px * NZ + z, py * 2 + core)

    def x_peer(i):
        return (mod(x + i, NX) * NZ + z, c_all)

    def rows_of(chip):
        return pl.ds(pl.multiple_of(chip * UNIT, UNIT), UNIT)

    def remote(src, dst, send, recv, device):
        return pltpu.make_async_remote_copy(
            src_ref=src, dst_ref=dst, send_sem=send, recv_sem=recv,
            device_id=device, device_id_type=MESH,
        )

    def own_tokens(c):
        return pltpu.make_async_copy(tokens.at[:, pl.ds(c * COLS, COLS)], tok.at[z, c], in_sem)

    routing = ((ids_in, ids), (probs_in, probs), (limit_in, limit))
    for i, (src, dst) in enumerate(routing):
        pltpu.make_async_copy(src, dst, route_sem.at[i]).start()
    for c in range(CHUNKS):
        own_tokens(c).start()
    wide = pl.ds(pl.multiple_of(core * (HIDDEN // 2), HIDDEN // 2), HIDDEN // 2)
    other = pl.ds(pl.multiple_of((1 - core) * (HIDDEN // 2), HIDDEN // 2), HIDDEN // 2)
    weights = (
        (gate.at[0], gw.at[:, wide]), (up.at[0], uw.at[:, wide]), (down.at[0], dw.at[wide, :]),
    )
    theirs = (gw.at[:, other], uw.at[:, other], dw.at[other, :])
    barrier = pltpu.get_barrier_semaphore()
    pl.semaphore_signal(barrier, inc=1, device_id=partner, device_id_type=MESH)

    def greet_z(i, carry):
        pl.semaphore_signal(barrier, inc=1, device_id=z_peer(i), device_id_type=MESH)
        return carry

    def greet_xy(i, carry):
        pl.semaphore_signal(barrier, inc=1, device_id=xy_peer(i)[1], device_id_type=MESH)
        return carry

    lax.fori_loop(1, NZ, greet_z, 0)
    lax.fori_loop(1, PEERS, greet_xy, 0)

    col = lax.broadcasted_iota(jnp.int32, (EXPERTS, TOK), 1)
    row = lax.broadcasted_iota(jnp.int32, (EXPERTS, TOK), 0)
    for i, (src, dst) in enumerate(routing):
        pltpu.make_async_copy(src, dst, route_sem.at[i]).wait()
    chosen = jnp.zeros((EXPERTS, TOK), F32)
    weight = jnp.zeros((EXPERTS, TOK), F32)
    for k in range(8):
        hit = ids[k : k + 1, :] == row
        chosen = jnp.where(hit, 1.0, chosen)
        weight = jnp.where(hit, probs[k : k + 1, :], weight)
    earlier = jnp.where(row < col, 1.0, 0.0).astype(BF)
    rank = jnp.dot(chosen.astype(BF), earlier, preferred_element_type=F32)
    rank = jnp.where(chosen > 0.5, rank, 1000.0).T
    weight = weight.T
    rank = jnp.where(rank < limit[...].astype(F32), rank, 1000.0)
    token_id = row.astype(F32)
    for r in range(SLOTS):
        at = rank == float(r)
        meta[z, r : r + 1, :] = jnp.sum(jnp.where(at, token_id + 1000.0, 0.0), axis=0, keepdims=True) - 1000.0
        meta[z, SLOTS + r : SLOTS + r + 1, :] = jnp.sum(jnp.where(at, weight, 0.0), axis=0, keepdims=True)

    def send_meta(i, carry):
        remote(meta.at[z], meta.at[z], meta_send, meta_recv, z_peer(i)).start()
        return carry


    def unit_of(hop, c):
        return c - 2 * div(hop, FAR) * (c // 2)

    def ag(way, hop, c):
        block = mod(z + NZ - hop + 1, NZ) if way == UP else mod(z + hop - 1, NZ)
        return remote(
            tok.at[block, c], tok.at[block, c], ag_send, ag_recv.at[hop - 1, unit_of(hop, c)],
            neighbour(way),
        )

    def ag_arrived(hop, c):
        two = tok.at[pl.ds(0, 2), c]
        remote(two, two, ag_send, ag_recv.at[hop - 1, c], z_peer(1)).wait_recv()

    def metas():
        several = meta.at[pl.ds(0, NZ - 1)]
        return remote(several, several, meta_send, meta_recv, z_peer(1))

    def some_totals():
        some = totals.at[pl.ds(0, NX - 1)]
        return remote(some, some, tot_send, tot_recv, x_peer(1))

    def count_of(s):
        return jnp.sum(jnp.where(meta[s, 0:SLOTS, :] >= 0.0, 1.0, 0.0), axis=0, keepdims=True)

    def send_totals():
        total = jnp.zeros((1, EXPERTS), F32)
        for s in range(NZ):
            total = total + count_of(s)
        totals[x] = jnp.broadcast_to(total, (8, EXPERTS))

        def send_total(i, carry):
            remote(totals.at[x], totals.at[x], tot_send, tot_recv, x_peer(i)).start()
            return carry

        lax.fori_loop(1, NX, send_total, 0)

    def pair(k):
        return mod(z + NZ - k, NZ), mod(z + k, NZ)

    def far_chunk(k, c):
        return c + 2 * (1 - div(mod(k, 4) + 3, 4))

    def slot_values(first, second):
        stacked = jnp.concatenate([first, second] * PEERS, axis=0)
        s = lax.broadcasted_iota(jnp.int32, (ROWS, EXPERTS), 0)
        e = lax.broadcasted_iota(jnp.int32, (ROWS, EXPERTS), 1)
        chip = s >> 4
        expert = (chip >> 2) * (NZ * NY) + z * NY + (chip & 3)
        return jnp.sum(jnp.where(e == expert, stacked, 0.0), axis=1, keepdims=True)

    def selection(k):
        a, b = pair(k)
        source = slot_values(meta[a, 0:SLOTS, :], meta[b, 0:SLOTS, :])
        s = lax.broadcasted_iota(jnp.int32, (ROWS, 2 * TOK), 0)
        t = lax.broadcasted_iota(jnp.int32, (ROWS, 2 * TOK), 1)
        second = (s >> 3) & 1
        return (t - second * TOK).astype(F32) == source

    def exchange(src, dst, send, recv, k, c):
        def one(i, carry):
            chip, device = xy_peer(PEERS - i)
            remote(src.at[k, c, rows_of(chip)], dst.at[k, c, rows_of(me)], send, recv.at[k, c], device).start()
            return carry

        lax.fori_loop(1, PEERS, one, 0)

    def half_of(h):
        return pl.ds(h * (COLS // 2), COLS // 2)

    def exchange_half(h):
        def one(i, carry):
            chip, device = xy_peer(PEERS - i)
            remote(
                obuf.at[FAR - 1, 0, rows_of(chip), half_of(h)], ybuf.at[FAR - 1, 0, rows_of(me), half_of(h)],
                r_send, r_recv.at[0, 2 + h], device,
            ).start()
            return carry

        lax.fori_loop(1, PEERS, one, 0)

    def exchanged(src, dst, send, recv, k, c):
        most = pl.ds(0, (PEERS - 1) * UNIT)
        return remote(src.at[k, c, most], dst.at[k, c, most], send, recv.at[k, c], x_peer(1))

    def pick_rows(k, c):
        a, b = pair(k)
        both = jnp.concatenate([tok[a, c], tok[b, far_chunk(k, c)]], axis=0)
        sbuf[k, c] = jnp.dot(mix[k], both, preferred_element_type=F32).astype(BF)
        rbuf[k, c, rows_of(me), :] = sbuf[k, c, rows_of(me), :]

    def dispatch(k, c):
        ag_arrived(k, c)
        if c < 2:
            pl.when(k < FAR)(lambda: ag(UP, k + 1, c).start())
            pl.when(k < FAR - 1)(lambda: ag(DOWN, k + 1, c).start())
        else:
            pl.when(k < FAR - 1)(lambda: ag(UP, k + 1, c).start())
            ag(DOWN, k + 1, c).start()
        pick_rows(k, c)
        exchange(sbuf, rbuf, d_send, d_recv, k, c)

    second_half = (lax.broadcasted_iota(jnp.int32, (ROWS, 256), 0) >> 3) & 1
    second_wide = (lax.broadcasted_iota(jnp.int32, (ROWS, COLS), 0) >> 3) & 1

    def block(c):
        return slice(c * COLS, (c + 1) * COLS)

    def split_k(k):
        return (k > 0) & (k < FAR)

    def arrived(k, c):
        exchanged(sbuf, rbuf, d_send, d_recv, k, c).wait_recv()

    def add_chunk(k, c, spread, fresh):
        arrived(k, c)
        for total, w in ((gate_sum, gw), (up_sum, uw)):
            for n in range(0, HIDDEN, 256):
                cols = slice(n, n + 256)
                value = jnp.dot(rbuf[k, c], w[block(c), cols], preferred_element_type=F32)
                if spread:
                    right = jnp.dot(rbuf[k, c], w[block(c + 2), cols], preferred_element_type=F32)
                    value = jnp.where(second_half == 0, value, right)
                total[:, cols] = value if fresh else total[:, cols] + value

    def activate(spread):
        for n in range(0, HIDDEN, 256):
            cols = slice(n, n + 256)
            values = []
            for total in (gate_sum, up_sum):
                value = total[:, cols]
                if spread:
                    value = value + jnp.where(
                        second_half == 0, pltpu.roll(value, ROWS - SLOTS, 0), pltpu.roll(value, SLOTS, 0)
                    )
                values.append(value)
            gv, uv = values
            hid[:, cols] = (gv / (1.0 + jnp.exp(-gv)) * uv).astype(BF)

    def outputs(k):
        for c in range(2):
            left, right = (
                jnp.dot(hid[...], dw[:, block(chunk)], preferred_element_type=F32) for chunk in (c, c + 2)
            )
            obuf[k, c] = jnp.where(second_wide == 0, left, right).astype(BF)
            ybuf[k, c, rows_of(me), :] = obuf[k, c, rows_of(me), :]

            @pl.when(split_k(k))
            def _():
                obuf[k, c + 2] = jnp.where(second_wide == 0, right, left).astype(BF)
                ybuf[k, c + 2, rows_of(me), :] = obuf[k, c + 2, rows_of(me), :]

    def weights_here():
        for i, (src, dst) in enumerate(weights):
            pltpu.make_async_copy(src, dst, w_loc.at[i]).wait()
            remote(src, theirs[i], w_send.at[i], w_recv.at[i], partner).wait_recv()

    def weigh_all():
        some_totals().wait_recv()
        before_x = jnp.zeros((1, EXPERTS), F32)
        for s in range(NX):
            before_x = before_x + jnp.where(s < x, 1.0, 0.0) * totals[s, 0:1, :]

        def kept_weight(shard):
            offset = before_x
            for s in range(NZ):
                offset = offset + jnp.where(s < shard, 1.0, 0.0) * count_of(s)
            r = lax.broadcasted_iota(jnp.int32, (SLOTS, EXPERTS), 0).astype(F32)
            return jnp.where(offset + r < float(COL_CAP), meta[shard, SLOTS : 2 * SLOTS, :], 0.0)

        def weigh(k, carry):
            a, b = pair(k)
            w = slot_values(kept_weight(a), kept_weight(b))
            mix[k] = jnp.where(selection(k), w, 0.0).T.astype(BF)
            return carry

        lax.fori_loop(0, FAR + 1, weigh, 0)

    def step(k, carry):
        @pl.when(k == 1)
        def _():
            metas().wait_recv()
            send_totals()

        @pl.when(k <= FAR)
        def _():
            mix[k] = jnp.where(selection(k), 1.0, 0.0).astype(BF)

        for c in range(CHUNKS):
            if c < 2:
                pl.when(k <= FAR)(lambda: dispatch(k, c))
            else:
                pl.when(split_k(k))(lambda: dispatch(k, c))
            if c < 2:
                pl.when((k > 1) & (k <= FAR))(lambda: add_chunk(k - 1, c + 1, False, False))
            if c == 2:
                @pl.when(k == 1)
                def _():
                    weights_here()
                    add_chunk(0, 0, True, True)
                    add_chunk(0, 1, True, False)
                    activate(True)

                @pl.when((k > 1) & (k <= FAR))
                def _():
                    add_chunk(k - 1, 3, False, False)
                    activate(False)

                @pl.when(k == FAR + 1)
                def _():
                    add_chunk(FAR, 1, True, False)
                    activate(True)

            if c == 3:
                outputs(k - 1)
                pl.when(k < FAR)(lambda: add_chunk(k, 0, False, True))

                @pl.when(k == FAR)
                def _():
                    for h in range(2):
                        exchange_half(h)
                    exchange(obuf, ybuf, r_send, r_recv, FAR - 1, 1)
                    weigh_all()
                    add_chunk(FAR, 0, True, True)

        return carry

    pltpu.make_async_copy(tok.at[z], tok.at[z], in_sem).wait()
    for i, (src, dst) in enumerate(weights):
        pltpu.make_async_copy(src, dst, w_loc.at[i]).start()
    mix[0] = jnp.where(selection(0), 1.0, 0.0).astype(BF)
    for c in range(2):
        pick_rows(0, c)

    pl.semaphore_wait(barrier, NZ - 1 + PEERS - 1 + 1)
    lax.fori_loop(1, NZ, send_meta, 0)
    for c in range(CHUNKS):
        for way in range(2):
            ag(way, 1, c).start()
        if c < 2:
            exchange(sbuf, rbuf, d_send, d_recv, 0, c)
    for i, (src, dst) in enumerate(weights):
        remote(src, dst, w_send.at[i], w_recv.at[i], partner).start()

    lax.fori_loop(1, FAR + 2, step, 0)
    for c in (0, 1):
        exchange(obuf, ybuf, r_send, r_recv, FAR, c)
    def rs(way, k, c):
        unit = c if way == DOWN else mod(c + 2, CHUNKS)
        return remote(
            rs_out.at[way, k - 1, c], rs_in.at[way, k - 1, c], rs_send, rs_recv.at[k - 1, unit], neighbour(way)
        )

    def rs_arrived(k, unit):
        two = rs_in.at[pl.ds(0, 2), k - 1, unit]
        remote(two, two, rs_send, rs_recv.at[k - 1, unit], z_peer(1)).wait_recv()

    def gather_part(k, c):
        exchanged(obuf, ybuf, r_send, r_recv, k, c).wait_recv()
        part[...] = jnp.dot(mix[k], ybuf[k, c], preferred_element_type=F32)

    def mine(way):
        return slice(TOK, 2 * TOK) if way == UP else slice(0, TOK)

    def chunk_of(way, c):
        return (c + 2) % CHUNKS if way == UP else c

    def pass_on(way, k, c):
        chunk = chunk_of(way, c)
        rs_out[way, k - 1, chunk] = (part[mine(way), :] + rs_in[way, k, chunk].astype(F32)).astype(BF)
        rs(way, k, chunk).start()

    def begin(c):
        gather_part(FAR - 1, c)
        if c >= 2:
            rs_arrived(FAR, c)
        for way in range(2):
            if c < 2:
                rs_out[way, FAR - 2, chunk_of(way, c)] = part[mine(way), :].astype(BF)
                rs(way, FAR - 1, chunk_of(way, c)).start()
            else:
                pass_on(way, FAR - 1, c)

    def begin_far(c):
        gather_part(FAR, c)
        for way in range(2):
            rs_out[way, FAR - 1, c + 2 * way] = part[way * TOK : (way + 1) * TOK, :].astype(BF)
            rs(way, FAR, c + 2 * way).start()

    for h in range(2):
        most = ybuf.at[FAR - 1, 0, pl.ds(0, (PEERS - 1) * UNIT), half_of(h)]
        remote(most, most, r_send, r_recv.at[0, 2 + h], x_peer(1)).wait_recv()
        cols = slice(h * (COLS // 2), (h + 1) * (COLS // 2))
        value = jnp.dot(mix[FAR - 1], ybuf[FAR - 1, 0, :, cols], preferred_element_type=F32)
        for way in range(2):
            chunk = chunk_of(way, 0)
            rs_out[way, FAR - 2, chunk, :, cols] = value[mine(way), :].astype(BF)
            remote(
                rs_out.at[way, FAR - 2, chunk, :, half_of(h)], rs_in.at[way, FAR - 2, chunk, :, half_of(h)],
                rs_send, rs_recv.at[FAR - 2, 0], neighbour(way),
            ).start()
    begin(1)
    for c in (2, 3):
        exchange(obuf, ybuf, r_send, r_recv, FAR - 1, c)
    begin_far(0)
    exchange(obuf, ybuf, r_send, r_recv, FAR - 2, 0)
    begin_far(1)
    exchange(obuf, ybuf, r_send, r_recv, FAR - 2, 1)
    for c in (2, 3):
        begin(c)
        exchange(obuf, ybuf, r_send, r_recv, FAR - 2, c)

    def collect(i, carry):
        k = FAR - 2 - i
        for c in range(CHUNKS):
            gather_part(k, c)
            rs_arrived(k + 1, c)
            for way in range(2):
                pass_on(way, k, c)
            if c < 2:
                exchange(obuf, ybuf, r_send, r_recv, k - 1, c)
            else:
                pl.when(k > 1)(lambda: exchange(obuf, ybuf, r_send, r_recv, k - 1, c))
        return carry

    lax.fori_loop(0, FAR - 2, collect, 0)
    for i, (src, dst) in enumerate(weights):
        remote(src, dst, w_send.at[i], w_recv.at[i], partner).wait_send()
    metas().wait_send()
    some_totals().wait_send()
    blocks = tok.at[pl.ds(0, NZ - 1)]
    remote(blocks, blocks, ag_send, ag_recv.at[0, 0], z_peer(1)).wait_send()
    rows = sbuf.at[pl.ds(0, FAR), :, pl.ds(0, (PEERS - 1) * UNIT)]
    remote(rows, rows, d_send, d_recv.at[0, 0], x_peer(1)).wait_send()

    for c in range(2):
        gather_part(0, c)
        for q in range(2):
            rs_arrived(1, c + 2 * q)
        for q in range(2):
            chunk = c + 2 * q
            out[:, block(chunk)] = (
                part[q * TOK : (q + 1) * TOK, :] + rs_in[UP, 0, chunk].astype(F32) + rs_in[DOWN, 0, chunk].astype(F32)
            ).astype(BF)

    remote(rows, rows, r_send, r_recv.at[0, 0], x_peer(1)).wait_send()
    sums = rs_out.at[:, :, :, pl.ds(0, TOK * (NZ - 1) // NZ)]
    remote(sums, sums, rs_send, rs_recv.at[0, 0], z_peer(1)).wait_send()


def on_device(tokens, expert_ids, route_probs, shard_limit, gate_proj, up_proj, down_proj):
    dma = pltpu.SemaphoreType.DMA
    anywhere = pl.BlockSpec(memory_space=pltpu.HBM)
    near = pl.BlockSpec(memory_space=pltpu.VMEM)
    unit = (FAR + 1, CHUNKS, ROWS, COLS)
    operands = (tokens, expert_ids.T, route_probs.T, shard_limit, gate_proj, up_proj, down_proj)
    ring = (2, FAR, CHUNKS)
    return pl.pallas_call(
        kernel,
        out_shape=jax.ShapeDtypeStruct((TOK, WIDTH), BF),
        in_specs=[anywhere] * len(operands),
        out_specs=near,
        scratch_shapes=[
            pltpu.VMEM((8, TOK), jnp.int32),
            pltpu.VMEM((8, TOK), F32),
            pltpu.VMEM((1, EXPERTS), jnp.int32),
            pltpu.VMEM((NZ, CHUNKS, TOK, COLS), BF),
            pltpu.VMEM((NZ, 2 * SLOTS, EXPERTS), F32),
            pltpu.VMEM((NX, 8, EXPERTS), F32),
            pltpu.VMEM((WIDTH, HIDDEN), BF),
            pltpu.VMEM((WIDTH, HIDDEN), BF),
            pltpu.VMEM((HIDDEN, WIDTH), BF),
            pltpu.VMEM(unit, BF),
            pltpu.VMEM(unit, BF),
            pltpu.VMEM((ROWS, HIDDEN), F32),
            pltpu.VMEM((ROWS, HIDDEN), F32),
            pltpu.VMEM((ROWS, HIDDEN), BF),
            pltpu.VMEM(unit, BF),
            pltpu.VMEM(unit, BF),
            pltpu.VMEM((FAR + 1, 2 * TOK, ROWS), BF),
            pltpu.VMEM((2 * TOK, COLS), F32),
            pltpu.VMEM((*ring, TOK, COLS), BF),
            pltpu.VMEM((*ring, TOK, COLS), BF),
            dma((3,)), dma, dma((3,)), dma((3,)), dma((3,)), dma, dma, dma, dma,
            dma, dma(ring[1:]), dma, dma(unit[:2]), dma, dma(unit[:2]), dma, dma(ring[1:]),
        ],
        compiler_params=pltpu.CompilerParams(
            collective_id=0, has_side_effects=True, vmem_limit_bytes=56000000
        ),
        name="expert_layer",
    )(*(pltpu.with_memory_space_constraint(array, pltpu.HBM) for array in operands))


def solution(mesh):
    whole = ("dp", "expert")
    in_specs = (
        P(whole, None), P(whole, None), P(whole, None), P(whole, None),
        P(whole, None, None), P(whole, None, None), P(whole, None, None),
    )
    return jax.shard_map(
        on_device, mesh=mesh, in_specs=in_specs, out_specs=P(whole, None), check_vma=False
    )
```

```python
import jax
import jax.numpy as jnp
from jax import lax
from jax.experimental import pallas as pl
from jax.experimental.pallas import tpu as pltpu
from jax.sharding import PartitionSpec as P

MESH = pl.DeviceIdType.MESH
BF = jnp.bfloat16
F32 = jnp.float32

NX, NY, NZ = 4, 4, 8
TOK = 128
SLOTS = 8
COL_CAP = 128
WIDTH = 2048
CHUNKS = 4
COLS = WIDTH // CHUNKS
HIDDEN = 768
PEERS = NX * NY
UNIT = 2 * SLOTS
ROWS = PEERS * UNIT
EXPERTS = 128
FAR = NZ // 2
UP, DOWN = 0, 1


def mod(a, n):
    return a % n if isinstance(a, int) else lax.rem(a, n)


def div(a, n):
    return a // n if isinstance(a, int) else lax.div(a, n)


def kernel(
    tokens, ids_in, probs_in, limit_in, gate, up, down, out,
    ids, probs, limit, tok, meta, totals, gw, uw, dw, sbuf, rbuf, gate_sum, up_sum, hid, obuf, ybuf, mix, back, part, rs_in, rs_out,
    route_sem, in_sem, w_loc, w_send, w_recv, meta_send, meta_recv, tot_send, tot_recv,
    ag_send, ag_recv, d_send, d_recv, r_send, r_recv, rs_send, rs_recv,
):
    d = lax.axis_index("dp")
    c_all = lax.axis_index("expert")
    x, z = div(d, NZ), mod(d, NZ)
    y, core = div(c_all, 2), mod(c_all, 2)
    me = x * NY + y
    partner = (d, y * 2 + (1 - core))

    def z_peer(step):
        return (x * NZ + mod(z + step, NZ), c_all)

    def neighbour(way):
        return z_peer(1 if way == UP else NZ - 1)

    def xy_peer(i):
        px, py = mod(x + mod(i, NX), NX), mod(y + div(i, NX), NY)
        return px * NY + py, (px * NZ + z, py * 2 + core)

    def x_peer(i):
        return (mod(x + i, NX) * NZ + z, c_all)

    def rows_of(chip):
        return pl.ds(pl.multiple_of(chip * UNIT, UNIT), UNIT)

    def remote(src, dst, send, recv, device):
        return pltpu.make_async_remote_copy(
            src_ref=src, dst_ref=dst, send_sem=send, recv_sem=recv,
            device_id=device, device_id_type=MESH,
        )

    def own_tokens(c):
        return pltpu.make_async_copy(tokens.at[:, pl.ds(c * COLS, COLS)], tok.at[z, c], in_sem)

    routing = ((ids_in, ids), (probs_in, probs), (limit_in, limit))
    for i, (src, dst) in enumerate(routing):
        pltpu.make_async_copy(src, dst, route_sem.at[i]).start()
    for c in range(CHUNKS):
        own_tokens(c).start()
    wide = pl.ds(pl.multiple_of(core * (HIDDEN // 2), HIDDEN // 2), HIDDEN // 2)
    other = pl.ds(pl.multiple_of((1 - core) * (HIDDEN // 2), HIDDEN // 2), HIDDEN // 2)
    weights = (
        (gate.at[0], gw.at[:, wide]), (up.at[0], uw.at[:, wide]), (down.at[0], dw.at[wide, :]),
    )
    theirs = (gw.at[:, other], uw.at[:, other], dw.at[other, :])
    barrier = pltpu.get_barrier_semaphore()
    pl.semaphore_signal(barrier, inc=1, device_id=partner, device_id_type=MESH)

    def greet_z(i, carry):
        pl.semaphore_signal(barrier, inc=1, device_id=z_peer(i), device_id_type=MESH)
        return carry

    def greet_xy(i, carry):
        pl.semaphore_signal(barrier, inc=1, device_id=xy_peer(i)[1], device_id_type=MESH)
        return carry

    lax.fori_loop(1, NZ, greet_z, 0)
    lax.fori_loop(1, PEERS, greet_xy, 0)

    col = lax.broadcasted_iota(jnp.int32, (EXPERTS, TOK), 1)
    row = lax.broadcasted_iota(jnp.int32, (EXPERTS, TOK), 0)
    for i, (src, dst) in enumerate(routing):
        pltpu.make_async_copy(src, dst, route_sem.at[i]).wait()
    chosen = jnp.zeros((EXPERTS, TOK), F32)
    weight = jnp.zeros((EXPERTS, TOK), F32)
    for k in range(8):
        hit = ids[k : k + 1, :] == row
        chosen = jnp.where(hit, 1.0, chosen)
        weight = jnp.where(hit, probs[k : k + 1, :], weight)
    earlier = jnp.where(row < col, 1.0, 0.0).astype(BF)
    rank = jnp.dot(chosen.astype(BF), earlier, preferred_element_type=F32)
    rank = jnp.where(chosen > 0.5, rank, 1000.0).T
    weight = weight.T
    rank = jnp.where(rank < limit[...].astype(F32), rank, 1000.0)
    token_id = row.astype(F32)
    for r in range(SLOTS):
        at = rank == float(r)
        meta[z, r : r + 1, :] = jnp.sum(jnp.where(at, token_id + 1000.0, 0.0), axis=0, keepdims=True) - 1000.0
        meta[z, SLOTS + r : SLOTS + r + 1, :] = jnp.sum(jnp.where(at, weight, 0.0), axis=0, keepdims=True)

    def send_meta(i, carry):
        remote(meta.at[z], meta.at[z], meta_send, meta_recv, z_peer(i)).start()
        return carry


    def unit_of(hop, c):
        return c - 2 * div(hop, FAR) * (c // 2)

    def ag(way, hop, c):
        block = mod(z + NZ - hop + 1, NZ) if way == UP else mod(z + hop - 1, NZ)
        return remote(
            tok.at[block, c], tok.at[block, c], ag_send, ag_recv.at[hop - 1, unit_of(hop, c)],
            neighbour(way),
        )

    def ag_arrived(hop, c):
        two = tok.at[pl.ds(0, 2), c]
        remote(two, two, ag_send, ag_recv.at[hop - 1, c], z_peer(1)).wait_recv()

    def metas():
        several = meta.at[pl.ds(0, NZ - 1)]
        return remote(several, several, meta_send, meta_recv, z_peer(1))

    def some_totals():
        some = totals.at[pl.ds(0, NX - 1)]
        return remote(some, some, tot_send, tot_recv, x_peer(1))

    def count_of(s):
        return jnp.sum(jnp.where(meta[s, 0:SLOTS, :] >= 0.0, 1.0, 0.0), axis=0, keepdims=True)

    def send_totals():
        total = jnp.zeros((1, EXPERTS), F32)
        for s in range(NZ):
            total = total + count_of(s)
        totals[x] = jnp.broadcast_to(total, (8, EXPERTS))

        def send_total(i, carry):
            remote(totals.at[x], totals.at[x], tot_send, tot_recv, x_peer(i)).start()
            return carry

        lax.fori_loop(1, NX, send_total, 0)

    def pair(k):
        return mod(z + NZ - k, NZ), mod(z + k, NZ)

    def far_chunk(k, c):
        return c + 2 * (1 - div(mod(k, 4) + 3, 4))

    def slot_values(first, second):
        stacked = jnp.concatenate([first, second] * PEERS, axis=0)
        s = lax.broadcasted_iota(jnp.int32, (ROWS, EXPERTS), 0)
        e = lax.broadcasted_iota(jnp.int32, (ROWS, EXPERTS), 1)
        chip = s >> 4
        expert = (chip >> 2) * (NZ * NY) + z * NY + (chip & 3)
        return jnp.sum(jnp.where(e == expert, stacked, 0.0), axis=1, keepdims=True)

    def selection(k):
        a, b = pair(k)
        source = slot_values(meta[a, 0:SLOTS, :], meta[b, 0:SLOTS, :])
        s = lax.broadcasted_iota(jnp.int32, (ROWS, 2 * TOK), 0)
        t = lax.broadcasted_iota(jnp.int32, (ROWS, 2 * TOK), 1)
        second = (s >> 3) & 1
        return (t - second * TOK).astype(F32) == source

    def exchange(src, dst, send, recv, k, c):
        def one(i, carry):
            chip, device = xy_peer(PEERS - i)
            remote(src.at[k, c, rows_of(chip)], dst.at[k, c, rows_of(me)], send, recv.at[k, c], device).start()
            return carry

        lax.fori_loop(1, PEERS, one, 0)

    def half_of(h):
        return pl.ds(h * (COLS // 2), COLS // 2)

    def exchange_half(h):
        def one(i, carry):
            chip, device = xy_peer(PEERS - i)
            remote(
                obuf.at[FAR - 1, 0, rows_of(chip), half_of(h)], ybuf.at[FAR - 1, 0, rows_of(me), half_of(h)],
                r_send, r_recv.at[0, 2 + h], device,
            ).start()
            return carry

        lax.fori_loop(1, PEERS, one, 0)

    def exchanged(src, dst, send, recv, k, c):
        most = pl.ds(0, (PEERS - 1) * UNIT)
        return remote(src.at[k, c, most], dst.at[k, c, most], send, recv.at[k, c], x_peer(1))

    def pick_rows(k, c):
        a, b = pair(k)
        both = jnp.concatenate([tok[a, c], tok[b, far_chunk(k, c)]], axis=0)
        sbuf[k, c] = jnp.dot(mix[k], both, preferred_element_type=F32).astype(BF)
        rbuf[k, c, rows_of(me), :] = sbuf[k, c, rows_of(me), :]

    def dispatch(k, c):
        ag_arrived(k, c)
        if c < 2:
            pl.when(k < FAR)(lambda: ag(UP, k + 1, c).start())
            pl.when(k < FAR - 1)(lambda: ag(DOWN, k + 1, c).start())
        else:
            pl.when(k < FAR - 1)(lambda: ag(UP, k + 1, c).start())
            ag(DOWN, k + 1, c).start()
        pick_rows(k, c)
        exchange(sbuf, rbuf, d_send, d_recv, k, c)

    second_half = (lax.broadcasted_iota(jnp.int32, (ROWS, 256), 0) >> 3) & 1
    second_wide = (lax.broadcasted_iota(jnp.int32, (ROWS, COLS), 0) >> 3) & 1

    def block(c):
        return slice(c * COLS, (c + 1) * COLS)

    def split_k(k):
        return (k > 0) & (k < FAR)

    def arrived(k, c):
        exchanged(sbuf, rbuf, d_send, d_recv, k, c).wait_recv()

    def add_chunk(k, c, spread, fresh):
        arrived(k, c)
        for total, w in ((gate_sum, gw), (up_sum, uw)):
            for n in range(0, HIDDEN, 256):
                cols = slice(n, n + 256)
                value = jnp.dot(rbuf[k, c], w[block(c), cols], preferred_element_type=F32)
                if spread:
                    right = jnp.dot(rbuf[k, c], w[block(c + 2), cols], preferred_element_type=F32)
                    value = jnp.where(second_half == 0, value, right)
                total[:, cols] = value if fresh else total[:, cols] + value

    def activate(spread):
        for n in range(0, HIDDEN, 256):
            cols = slice(n, n + 256)
            values = []
            for total in (gate_sum, up_sum):
                value = total[:, cols]
                if spread:
                    value = value + jnp.where(
                        second_half == 0, pltpu.roll(value, ROWS - SLOTS, 0), pltpu.roll(value, SLOTS, 0)
                    )
                values.append(value)
            gv, uv = values
            hid[:, cols] = (gv / (1.0 + jnp.exp(-gv)) * uv).astype(BF)

    def outputs(k):
        for c in range(2):
            left, right = (
                jnp.dot(hid[...], dw[:, block(chunk)], preferred_element_type=F32) for chunk in (c, c + 2)
            )
            obuf[k, c] = jnp.where(second_wide == 0, left, right).astype(BF)
            ybuf[k, c, rows_of(me), :] = obuf[k, c, rows_of(me), :]

            @pl.when(split_k(k))
            def _():
                obuf[k, c + 2] = jnp.where(second_wide == 0, right, left).astype(BF)
                ybuf[k, c + 2, rows_of(me), :] = obuf[k, c + 2, rows_of(me), :]

    def weights_here():
        for i, (src, dst) in enumerate(weights):
            pltpu.make_async_copy(src, dst, w_loc.at[i]).wait()
            remote(src, theirs[i], w_send.at[i], w_recv.at[i], partner).wait_recv()

    def weigh(first, last):
        before_x = jnp.zeros((1, EXPERTS), F32)
        for s in range(NX):
            before_x = before_x + jnp.where(s < x, 1.0, 0.0) * totals[s, 0:1, :]

        def kept_weight(shard):
            offset = before_x
            for s in range(NZ):
                offset = offset + jnp.where(s < shard, 1.0, 0.0) * count_of(s)
            r = lax.broadcasted_iota(jnp.int32, (SLOTS, EXPERTS), 0).astype(F32)
            return jnp.where(offset + r < float(COL_CAP), meta[shard, SLOTS : 2 * SLOTS, :], 0.0)

        def one(k, carry):
            a, b = pair(k)
            w = slot_values(kept_weight(a), kept_weight(b))
            back[k] = jnp.where(selection(k), w, 0.0).T.astype(BF)
            return carry

        lax.fori_loop(first, last, one, 0)

    def step(k, carry):
        @pl.when(k == 1)
        def _():
            metas().wait_recv()
            send_totals()

        @pl.when(k <= FAR)
        def _():
            mix[k] = jnp.where(selection(k), 1.0, 0.0).astype(BF)

        for c in range(CHUNKS):
            if c < 2:
                pl.when(k <= FAR)(lambda: dispatch(k, c))
            else:
                pl.when(split_k(k))(lambda: dispatch(k, c))
            if c < 2:
                pl.when((k > 1) & (k <= FAR))(lambda: add_chunk(k - 1, c + 1, False, False))
            if c == 1:
                pl.when(k == 2)(lambda: some_totals().wait_recv())
                pl.when((k > 1) & (k < FAR))(lambda: weigh(2 * k - 4, 2 * k - 2))
                pl.when(k == FAR)(lambda: weigh(FAR, FAR + 1))
            if c == 2:
                @pl.when(k == 1)
                def _():
                    weights_here()
                    add_chunk(0, 0, True, True)
                    add_chunk(0, 1, True, False)
                    activate(True)

                @pl.when((k > 1) & (k <= FAR))
                def _():
                    add_chunk(k - 1, 3, False, False)
                    activate(False)

                @pl.when(k == FAR + 1)
                def _():
                    add_chunk(FAR, 1, True, False)
                    activate(True)

            if c == 3:
                outputs(k - 1)
                pl.when(k < FAR)(lambda: add_chunk(k, 0, False, True))

                @pl.when(k == FAR)
                def _():
                    for h in range(2):
                        exchange_half(h)
                    exchange(obuf, ybuf, r_send, r_recv, FAR - 1, 1)
                    add_chunk(FAR, 0, True, True)

        return carry

    pltpu.make_async_copy(tok.at[z], tok.at[z], in_sem).wait()
    for i, (src, dst) in enumerate(weights):
        pltpu.make_async_copy(src, dst, w_loc.at[i]).start()
    mix[0] = jnp.where(selection(0), 1.0, 0.0).astype(BF)
    for c in range(2):
        pick_rows(0, c)

    pl.semaphore_wait(barrier, NZ - 1 + PEERS - 1 + 1)
    lax.fori_loop(1, NZ, send_meta, 0)
    for c in range(CHUNKS):
        for way in range(2):
            ag(way, 1, c).start()
        if c < 2:
            exchange(sbuf, rbuf, d_send, d_recv, 0, c)
    for i, (src, dst) in enumerate(weights):
        remote(src, dst, w_send.at[i], w_recv.at[i], partner).start()

    lax.fori_loop(1, FAR + 2, step, 0)
    def rs(way, k, c):
        unit = c if way == DOWN else mod(c + 2, CHUNKS)
        return remote(
            rs_out.at[way, k - 1, c], rs_in.at[way, k - 1, c], rs_send, rs_recv.at[k - 1, unit], neighbour(way)
        )

    def rs_arrived(k, unit):
        two = rs_in.at[pl.ds(0, 2), k - 1, unit]
        remote(two, two, rs_send, rs_recv.at[k - 1, unit], z_peer(1)).wait_recv()

    def gather_part(k, c):
        exchanged(obuf, ybuf, r_send, r_recv, k, c).wait_recv()
        part[...] = jnp.dot(back[k], ybuf[k, c], preferred_element_type=F32)

    def mine(way):
        return slice(TOK, 2 * TOK) if way == UP else slice(0, TOK)

    def chunk_of(way, c):
        return (c + 2) % CHUNKS if way == UP else c

    def pass_on(way, k, c):
        chunk = chunk_of(way, c)
        rs_out[way, k - 1, chunk] = (part[mine(way), :] + rs_in[way, k, chunk].astype(F32)).astype(BF)
        rs(way, k, chunk).start()

    def begin(c):
        gather_part(FAR - 1, c)
        if c >= 2:
            rs_arrived(FAR, c)
        for way in range(2):
            if c < 2:
                rs_out[way, FAR - 2, chunk_of(way, c)] = part[mine(way), :].astype(BF)
                rs(way, FAR - 1, chunk_of(way, c)).start()
            else:
                pass_on(way, FAR - 1, c)

    def begin_far(c):
        gather_part(FAR, c)
        for way in range(2):
            rs_out[way, FAR - 1, c + 2 * way] = part[way * TOK : (way + 1) * TOK, :].astype(BF)
            rs(way, FAR, c + 2 * way).start()

    for h in range(2):
        most = ybuf.at[FAR - 1, 0, pl.ds(0, (PEERS - 1) * UNIT), half_of(h)]
        remote(most, most, r_send, r_recv.at[0, 2 + h], x_peer(1)).wait_recv()
        cols = slice(h * (COLS // 2), (h + 1) * (COLS // 2))
        value = jnp.dot(back[FAR - 1], ybuf[FAR - 1, 0, :, cols], preferred_element_type=F32)
        for way in range(2):
            chunk = chunk_of(way, 0)
            rs_out[way, FAR - 2, chunk, :, cols] = value[mine(way), :].astype(BF)
            remote(
                rs_out.at[way, FAR - 2, chunk, :, half_of(h)], rs_in.at[way, FAR - 2, chunk, :, half_of(h)],
                rs_send, rs_recv.at[FAR - 2, 0], neighbour(way),
            ).start()
        exchange(obuf, ybuf, r_send, r_recv, FAR, h)
    begin(1)
    for c in (2, 3):
        exchange(obuf, ybuf, r_send, r_recv, FAR - 1, c)
    begin_far(0)
    exchange(obuf, ybuf, r_send, r_recv, FAR - 2, 0)
    begin_far(1)
    exchange(obuf, ybuf, r_send, r_recv, FAR - 2, 1)
    for c in (2, 3):
        begin(c)
        exchange(obuf, ybuf, r_send, r_recv, FAR - 2, c)

    def collect(i, carry):
        k = FAR - 2 - i
        for c in range(CHUNKS):
            gather_part(k, c)
            rs_arrived(k + 1, c)
            for way in range(2):
                pass_on(way, k, c)
            if c < 2:
                exchange(obuf, ybuf, r_send, r_recv, k - 1, c)
            else:
                pl.when(k > 1)(lambda: exchange(obuf, ybuf, r_send, r_recv, k - 1, c))
        return carry

    lax.fori_loop(0, FAR - 2, collect, 0)
    for i, (src, dst) in enumerate(weights):
        remote(src, dst, w_send.at[i], w_recv.at[i], partner).wait_send()
    metas().wait_send()
    some_totals().wait_send()
    blocks = tok.at[pl.ds(0, NZ - 1)]
    remote(blocks, blocks, ag_send, ag_recv.at[0, 0], z_peer(1)).wait_send()
    rows = sbuf.at[pl.ds(0, FAR), :, pl.ds(0, (PEERS - 1) * UNIT)]
    remote(rows, rows, d_send, d_recv.at[0, 0], x_peer(1)).wait_send()

    for c in range(2):
        gather_part(0, c)
        for q in range(2):
            rs_arrived(1, c + 2 * q)
        for q in range(2):
            chunk = c + 2 * q
            out[:, block(chunk)] = (
                part[q * TOK : (q + 1) * TOK, :] + rs_in[UP, 0, chunk].astype(F32) + rs_in[DOWN, 0, chunk].astype(F32)
            ).astype(BF)

    remote(rows, rows, r_send, r_recv.at[0, 0], x_peer(1)).wait_send()
    sums = rs_out.at[:, :, :, pl.ds(0, TOK * (NZ - 1) // NZ)]
    remote(sums, sums, rs_send, rs_recv.at[0, 0], z_peer(1)).wait_send()


def on_device(tokens, expert_ids, route_probs, shard_limit, gate_proj, up_proj, down_proj):
    dma = pltpu.SemaphoreType.DMA
    anywhere = pl.BlockSpec(memory_space=pltpu.HBM)
    near = pl.BlockSpec(memory_space=pltpu.VMEM)
    unit = (FAR + 1, CHUNKS, ROWS, COLS)
    operands = (tokens, expert_ids.T, route_probs.T, shard_limit, gate_proj, up_proj, down_proj)
    ring = (2, FAR, CHUNKS)
    return pl.pallas_call(
        kernel,
        out_shape=jax.ShapeDtypeStruct((TOK, WIDTH), BF),
        in_specs=[anywhere] * len(operands),
        out_specs=near,
        scratch_shapes=[
            pltpu.VMEM((8, TOK), jnp.int32),
            pltpu.VMEM((8, TOK), F32),
            pltpu.VMEM((1, EXPERTS), jnp.int32),
            pltpu.VMEM((NZ, CHUNKS, TOK, COLS), BF),
            pltpu.VMEM((NZ, 2 * SLOTS, EXPERTS), F32),
            pltpu.VMEM((NX, 8, EXPERTS), F32),
            pltpu.VMEM((WIDTH, HIDDEN), BF),
            pltpu.VMEM((WIDTH, HIDDEN), BF),
            pltpu.VMEM((HIDDEN, WIDTH), BF),
            pltpu.VMEM(unit, BF),
            pltpu.VMEM(unit, BF),
            pltpu.VMEM((ROWS, HIDDEN), F32),
            pltpu.VMEM((ROWS, HIDDEN), F32),
            pltpu.VMEM((ROWS, HIDDEN), BF),
            pltpu.VMEM(unit, BF),
            pltpu.VMEM(unit, BF),
            pltpu.VMEM((FAR + 1, 2 * TOK, ROWS), BF),
            pltpu.VMEM((FAR + 1, 2 * TOK, ROWS), BF),
            pltpu.VMEM((2 * TOK, COLS), F32),
            pltpu.VMEM((*ring, TOK, COLS), BF),
            pltpu.VMEM((*ring, TOK, COLS), BF),
            dma((3,)), dma, dma((3,)), dma((3,)), dma((3,)), dma, dma, dma, dma,
            dma, dma(ring[1:]), dma, dma(unit[:2]), dma, dma(unit[:2]), dma, dma(ring[1:]),
        ],
        compiler_params=pltpu.CompilerParams(
            collective_id=0, has_side_effects=True, vmem_limit_bytes=56000000
        ),
        name="expert_layer",
    )(*(pltpu.with_memory_space_constraint(array, pltpu.HBM) for array in operands))


def solution(mesh):
    whole = ("dp", "expert")
    in_specs = (
        P(whole, None), P(whole, None), P(whole, None), P(whole, None),
        P(whole, None, None), P(whole, None, None), P(whole, None, None),
    )
    return jax.shard_map(
        on_device, mesh=mesh, in_specs=in_specs, out_specs=P(whole, None), check_vma=False
    )
```

```python
import jax
import jax.numpy as jnp
from jax import lax
from jax.experimental import pallas as pl
from jax.experimental.pallas import tpu as pltpu
from jax.sharding import PartitionSpec as P

MESH = pl.DeviceIdType.MESH
BF = jnp.bfloat16
F32 = jnp.float32

NX, NY, NZ = 4, 4, 8
TOK = 128
SLOTS = 8
COL_CAP = 128
WIDTH = 2048
CHUNKS = 4
COLS = WIDTH // CHUNKS
HIDDEN = 768
PEERS = NX * NY
UNIT = 2 * SLOTS
ROWS = PEERS * UNIT
EXPERTS = 128
FAR = NZ // 2
UP, DOWN = 0, 1


def mod(a, n):
    return a % n if isinstance(a, int) else lax.rem(a, n)


def div(a, n):
    return a // n if isinstance(a, int) else lax.div(a, n)


def kernel(
    tokens, ids_in, probs_in, limit_in, gate, up, down, out,
    ids, probs, limit, tok, meta, totals, gw, uw, dw, sbuf, rbuf, gate_sum, up_sum, hid, obuf, ybuf, mix, back, part, rs_in, rs_out,
    route_sem, in_sem, w_loc, w_send, w_recv, meta_send, meta_recv, tot_send, tot_recv,
    ag_send, ag_recv, d_send, d_recv, r_send, r_recv, rs_send, rs_recv,
):
    d = lax.axis_index("dp")
    c_all = lax.axis_index("expert")
    x, z = div(d, NZ), mod(d, NZ)
    y, core = div(c_all, 2), mod(c_all, 2)
    me = x * NY + y
    partner = (d, y * 2 + (1 - core))

    def z_peer(step):
        return (x * NZ + mod(z + step, NZ), c_all)

    def neighbour(way):
        return z_peer(1 if way == UP else NZ - 1)

    def xy_peer(i):
        px, py = mod(x + mod(i, NX), NX), mod(y + div(i, NX), NY)
        return px * NY + py, (px * NZ + z, py * 2 + core)

    def x_peer(i):
        return (mod(x + i, NX) * NZ + z, c_all)

    def rows_of(chip):
        return pl.ds(pl.multiple_of(chip * UNIT, UNIT), UNIT)

    def remote(src, dst, send, recv, device):
        return pltpu.make_async_remote_copy(
            src_ref=src, dst_ref=dst, send_sem=send, recv_sem=recv,
            device_id=device, device_id_type=MESH,
        )

    def own_tokens(c):
        return pltpu.make_async_copy(tokens.at[:, pl.ds(c * COLS, COLS)], tok.at[z, c], in_sem)

    routing = ((ids_in, ids), (probs_in, probs), (limit_in, limit))
    for i, (src, dst) in enumerate(routing):
        pltpu.make_async_copy(src, dst, route_sem.at[i]).start()
    for c in range(CHUNKS):
        own_tokens(c).start()
    wide = pl.ds(pl.multiple_of(core * (HIDDEN // 2), HIDDEN // 2), HIDDEN // 2)
    other = pl.ds(pl.multiple_of((1 - core) * (HIDDEN // 2), HIDDEN // 2), HIDDEN // 2)
    weights = (
        (gate.at[0], gw.at[:, wide]), (up.at[0], uw.at[:, wide]), (down.at[0], dw.at[wide, :]),
    )
    theirs = (gw.at[:, other], uw.at[:, other], dw.at[other, :])
    barrier = pltpu.get_barrier_semaphore()
    pl.semaphore_signal(barrier, inc=1, device_id=partner, device_id_type=MESH)

    def greet_z(i, carry):
        pl.semaphore_signal(barrier, inc=1, device_id=z_peer(i), device_id_type=MESH)
        return carry

    def greet_xy(i, carry):
        pl.semaphore_signal(barrier, inc=1, device_id=xy_peer(i)[1], device_id_type=MESH)
        return carry

    lax.fori_loop(1, NZ, greet_z, 0)
    lax.fori_loop(1, PEERS, greet_xy, 0)

    col = lax.broadcasted_iota(jnp.int32, (EXPERTS, TOK), 1)
    row = lax.broadcasted_iota(jnp.int32, (EXPERTS, TOK), 0)
    for i, (src, dst) in enumerate(routing):
        pltpu.make_async_copy(src, dst, route_sem.at[i]).wait()
    chosen = jnp.zeros((EXPERTS, TOK), F32)
    weight = jnp.zeros((EXPERTS, TOK), F32)
    for k in range(8):
        hit = ids[k : k + 1, :] == row
        chosen = jnp.where(hit, 1.0, chosen)
        weight = jnp.where(hit, probs[k : k + 1, :], weight)
    earlier = jnp.where(row < col, 1.0, 0.0).astype(BF)
    rank = jnp.dot(chosen.astype(BF), earlier, preferred_element_type=F32)
    rank = jnp.where(chosen > 0.5, rank, 1000.0).T
    weight = weight.T
    rank = jnp.where(rank < limit[...].astype(F32), rank, 1000.0)
    token_id = row.astype(F32)
    for r in range(SLOTS):
        at = rank == float(r)
        meta[z, r : r + 1, :] = jnp.sum(jnp.where(at, token_id + 1000.0, 0.0), axis=0, keepdims=True) - 1000.0
        meta[z, SLOTS + r : SLOTS + r + 1, :] = jnp.sum(jnp.where(at, weight, 0.0), axis=0, keepdims=True)

    def send_metas():
        for i in (1, 7, 2, 6, 3, 5, 4):
            remote(meta.at[z], meta.at[z], meta_send, meta_recv.at[min(i, NZ - i) - 1], z_peer(i)).start()

    def unit_of(hop, c):
        return c - 2 * div(hop, FAR) * (c // 2)

    def ag(way, hop, c):
        block = mod(z + NZ - hop + 1, NZ) if way == UP else mod(z + hop - 1, NZ)
        return remote(
            tok.at[block, c], tok.at[block, c], ag_send, ag_recv.at[hop - 1, unit_of(hop, c)],
            neighbour(way),
        )

    def ag_arrived(hop, c):
        two = tok.at[pl.ds(0, 2), c]
        remote(two, two, ag_send, ag_recv.at[hop - 1, c], z_peer(1)).wait_recv()

    def metas(k, number):
        several = meta.at[pl.ds(0, number)]
        return remote(several, several, meta_send, meta_recv.at[k - 1], z_peer(1))

    def some_totals():
        some = totals.at[pl.ds(0, NX - 1)]
        return remote(some, some, tot_send, tot_recv, x_peer(1))

    def count_of(s):
        return jnp.sum(jnp.where(meta[s, 0:SLOTS, :] >= 0.0, 1.0, 0.0), axis=0, keepdims=True)

    def send_totals():
        total = jnp.zeros((1, EXPERTS), F32)
        for s in range(NZ):
            total = total + count_of(s)
        totals[x] = jnp.broadcast_to(total, (8, EXPERTS))

        def send_total(i, carry):
            remote(totals.at[x], totals.at[x], tot_send, tot_recv, x_peer(i)).start()
            return carry

        lax.fori_loop(1, NX, send_total, 0)

    def pair(k):
        return mod(z + NZ - k, NZ), mod(z + k, NZ)

    def far_chunk(k, c):
        return c + 2 * (1 - div(mod(k, 4) + 3, 4))

    def slot_values(first, second):
        stacked = jnp.concatenate([first, second] * PEERS, axis=0)
        s = lax.broadcasted_iota(jnp.int32, (ROWS, EXPERTS), 0)
        e = lax.broadcasted_iota(jnp.int32, (ROWS, EXPERTS), 1)
        chip = s >> 4
        expert = (chip >> 2) * (NZ * NY) + z * NY + (chip & 3)
        return jnp.sum(jnp.where(e == expert, stacked, 0.0), axis=1, keepdims=True)

    def selection(k):
        a, b = pair(k)
        source = slot_values(meta[a, 0:SLOTS, :], meta[b, 0:SLOTS, :])
        s = lax.broadcasted_iota(jnp.int32, (ROWS, 2 * TOK), 0)
        t = lax.broadcasted_iota(jnp.int32, (ROWS, 2 * TOK), 1)
        second = (s >> 3) & 1
        return (t - second * TOK).astype(F32) == source

    def exchange(src, dst, send, recv, k, c):
        def one(i, carry):
            chip, device = xy_peer(PEERS - i)
            remote(src.at[k, c, rows_of(chip)], dst.at[k, c, rows_of(me)], send, recv.at[k, c], device).start()
            return carry

        lax.fori_loop(1, PEERS, one, 0)

    def half_of(h):
        return pl.ds(h * (COLS // 2), COLS // 2)

    def exchange_half(h):
        def one(i, carry):
            chip, device = xy_peer(PEERS - i)
            remote(
                obuf.at[FAR - 1, 0, rows_of(chip), half_of(h)], ybuf.at[FAR - 1, 0, rows_of(me), half_of(h)],
                r_send, r_recv.at[0, 2 + h], device,
            ).start()
            return carry

        lax.fori_loop(1, PEERS, one, 0)

    def exchanged(src, dst, send, recv, k, c):
        most = pl.ds(0, (PEERS - 1) * UNIT)
        return remote(src.at[k, c, most], dst.at[k, c, most], send, recv.at[k, c], x_peer(1))

    def pick_rows(k, c):
        a, b = pair(k)
        both = jnp.concatenate([tok[a, c], tok[b, far_chunk(k, c)]], axis=0)
        sbuf[k, c] = jnp.dot(mix[k], both, preferred_element_type=F32).astype(BF)
        rbuf[k, c, rows_of(me), :] = sbuf[k, c, rows_of(me), :]

    def dispatch(k, c):
        ag_arrived(k, c)
        if c < 2:
            pl.when(k < FAR)(lambda: ag(UP, k + 1, c).start())
            pl.when(k < FAR - 1)(lambda: ag(DOWN, k + 1, c).start())
        else:
            pl.when(k < FAR - 1)(lambda: ag(UP, k + 1, c).start())
            ag(DOWN, k + 1, c).start()
        pick_rows(k, c)
        exchange(sbuf, rbuf, d_send, d_recv, k, c)

    second_half = (lax.broadcasted_iota(jnp.int32, (ROWS, 256), 0) >> 3) & 1
    second_wide = (lax.broadcasted_iota(jnp.int32, (ROWS, COLS), 0) >> 3) & 1

    def block(c):
        return slice(c * COLS, (c + 1) * COLS)

    def split_k(k):
        return (k > 0) & (k < FAR)

    def arrived(k, c):
        exchanged(sbuf, rbuf, d_send, d_recv, k, c).wait_recv()

    def add_chunk(k, c, spread, fresh):
        arrived(k, c)
        for total, w in ((gate_sum, gw), (up_sum, uw)):
            for n in range(0, HIDDEN, 256):
                cols = slice(n, n + 256)
                value = jnp.dot(rbuf[k, c], w[block(c), cols], preferred_element_type=F32)
                if spread:
                    right = jnp.dot(rbuf[k, c], w[block(c + 2), cols], preferred_element_type=F32)
                    value = jnp.where(second_half == 0, value, right)
                total[:, cols] = value if fresh else total[:, cols] + value

    def activate(spread):
        for n in range(0, HIDDEN, 256):
            cols = slice(n, n + 256)
            values = []
            for total in (gate_sum, up_sum):
                value = total[:, cols]
                if spread:
                    value = value + jnp.where(
                        second_half == 0, pltpu.roll(value, ROWS - SLOTS, 0), pltpu.roll(value, SLOTS, 0)
                    )
                values.append(value)
            gv, uv = values
            hid[:, cols] = (gv / (1.0 + jnp.exp(-gv)) * uv).astype(BF)

    def outputs(k):
        for c in range(2):
            left, right = (
                jnp.dot(hid[...], dw[:, block(chunk)], preferred_element_type=F32) for chunk in (c, c + 2)
            )
            obuf[k, c] = jnp.where(second_wide == 0, left, right).astype(BF)
            ybuf[k, c, rows_of(me), :] = obuf[k, c, rows_of(me), :]

            @pl.when(split_k(k))
            def _():
                obuf[k, c + 2] = jnp.where(second_wide == 0, right, left).astype(BF)
                ybuf[k, c + 2, rows_of(me), :] = obuf[k, c + 2, rows_of(me), :]

    def weights_here():
        for i, (src, dst) in enumerate(weights):
            pltpu.make_async_copy(src, dst, w_loc.at[i]).wait()
            remote(src, theirs[i], w_send.at[i], w_recv.at[i], partner).wait_recv()

    def weigh(first, last):
        before_x = jnp.zeros((1, EXPERTS), F32)
        for s in range(NX):
            before_x = before_x + jnp.where(s < x, 1.0, 0.0) * totals[s, 0:1, :]

        def kept_weight(shard):
            offset = before_x
            for s in range(NZ):
                offset = offset + jnp.where(s < shard, 1.0, 0.0) * count_of(s)
            r = lax.broadcasted_iota(jnp.int32, (SLOTS, EXPERTS), 0).astype(F32)
            return jnp.where(offset + r < float(COL_CAP), meta[shard, SLOTS : 2 * SLOTS, :], 0.0)

        def one(k, carry):
            a, b = pair(k)
            w = slot_values(kept_weight(a), kept_weight(b))
            back[k] = jnp.where(selection(k), w, 0.0).T.astype(BF)
            return carry

        lax.fori_loop(first, last, one, 0)

    def step(k, carry):
        @pl.when(k == 1)
        def _():
            metas(1, 2).wait_recv()

        @pl.when(k == 2)
        def _():
            metas(2, 2).wait_recv()
            metas(3, 2).wait_recv()
            metas(FAR, 1).wait_recv()
            send_totals()

        @pl.when(k <= FAR)
        def _():
            mix[k] = jnp.where(selection(k), 1.0, 0.0).astype(BF)

        for c in range(CHUNKS):
            if c < 2:
                pl.when(k <= FAR)(lambda: dispatch(k, c))
            else:
                pl.when(split_k(k))(lambda: dispatch(k, c))
            if c < 2:
                pl.when((k > 1) & (k <= FAR))(lambda: add_chunk(k - 1, c + 1, False, False))
            if c == 1:
                pl.when(k == FAR - 1)(lambda: some_totals().wait_recv())
                pl.when(k == FAR - 1)(lambda: weigh(0, 3))
                pl.when(k == FAR)(lambda: weigh(3, FAR + 1))
            if c == 2:
                @pl.when(k == 1)
                def _():
                    weights_here()
                    add_chunk(0, 0, True, True)
                    add_chunk(0, 1, True, False)
                    activate(True)

                @pl.when((k > 1) & (k <= FAR))
                def _():
                    add_chunk(k - 1, 3, False, False)
                    activate(False)

                @pl.when(k == FAR + 1)
                def _():
                    add_chunk(FAR, 1, True, False)
                    activate(True)

            if c == 3:
                outputs(k - 1)
                pl.when(k < FAR)(lambda: add_chunk(k, 0, False, True))

                @pl.when(k == FAR)
                def _():
                    for h in range(2):
                        exchange_half(h)
                    exchange(obuf, ybuf, r_send, r_recv, FAR - 1, 1)
                    add_chunk(FAR, 0, True, True)

        return carry

    pltpu.make_async_copy(tok.at[z], tok.at[z], in_sem).wait()
    for i, (src, dst) in enumerate(weights):
        pltpu.make_async_copy(src, dst, w_loc.at[i]).start()
    mix[0] = jnp.where(selection(0), 1.0, 0.0).astype(BF)
    for c in range(2):
        pick_rows(0, c)

    pl.semaphore_wait(barrier, NZ - 1 + PEERS - 1 + 1)
    send_metas()
    for c in range(CHUNKS):
        for way in range(2):
            ag(way, 1, c).start()
        if c < 2:
            exchange(sbuf, rbuf, d_send, d_recv, 0, c)
    for i, (src, dst) in enumerate(weights):
        remote(src, dst, w_send.at[i], w_recv.at[i], partner).start()

    lax.fori_loop(1, FAR + 2, step, 0)
    def rs(way, k, c):
        unit = c if way == DOWN else mod(c + 2, CHUNKS)
        return remote(
            rs_out.at[way, k - 1, c], rs_in.at[way, k - 1, c], rs_send, rs_recv.at[k - 1, unit], neighbour(way)
        )

    def rs_arrived(k, unit):
        two = rs_in.at[pl.ds(0, 2), k - 1, unit]
        remote(two, two, rs_send, rs_recv.at[k - 1, unit], z_peer(1)).wait_recv()

    def gather_part(k, c):
        exchanged(obuf, ybuf, r_send, r_recv, k, c).wait_recv()
        part[...] = jnp.dot(back[k], ybuf[k, c], preferred_element_type=F32)

    def mine(way):
        return slice(TOK, 2 * TOK) if way == UP else slice(0, TOK)

    def chunk_of(way, c):
        return (c + 2) % CHUNKS if way == UP else c

    def pass_on(way, k, c):
        chunk = chunk_of(way, c)
        rs_out[way, k - 1, chunk] = (part[mine(way), :] + rs_in[way, k, chunk].astype(F32)).astype(BF)
        rs(way, k, chunk).start()

    def begin(c):
        gather_part(FAR - 1, c)
        if c >= 2:
            rs_arrived(FAR, c)
        for way in range(2):
            if c < 2:
                rs_out[way, FAR - 2, chunk_of(way, c)] = part[mine(way), :].astype(BF)
                rs(way, FAR - 1, chunk_of(way, c)).start()
            else:
                pass_on(way, FAR - 1, c)

    def begin_far(c):
        gather_part(FAR, c)
        for way in range(2):
            rs_out[way, FAR - 1, c + 2 * way] = part[way * TOK : (way + 1) * TOK, :].astype(BF)
            rs(way, FAR, c + 2 * way).start()

    for h in range(2):
        most = ybuf.at[FAR - 1, 0, pl.ds(0, (PEERS - 1) * UNIT), half_of(h)]
        remote(most, most, r_send, r_recv.at[0, 2 + h], x_peer(1)).wait_recv()
        cols = slice(h * (COLS // 2), (h + 1) * (COLS // 2))
        value = jnp.dot(back[FAR - 1], ybuf[FAR - 1, 0, :, cols], preferred_element_type=F32)
        for way in range(2):
            chunk = chunk_of(way, 0)
            rs_out[way, FAR - 2, chunk, :, cols] = value[mine(way), :].astype(BF)
            remote(
                rs_out.at[way, FAR - 2, chunk, :, half_of(h)], rs_in.at[way, FAR - 2, chunk, :, half_of(h)],
                rs_send, rs_recv.at[FAR - 2, 0], neighbour(way),
            ).start()
        exchange(obuf, ybuf, r_send, r_recv, FAR, h)
    begin(1)
    for c in (2, 3):
        exchange(obuf, ybuf, r_send, r_recv, FAR - 1, c)
    begin_far(0)
    exchange(obuf, ybuf, r_send, r_recv, FAR - 2, 0)
    begin_far(1)
    exchange(obuf, ybuf, r_send, r_recv, FAR - 2, 1)
    for c in (2, 3):
        begin(c)
        exchange(obuf, ybuf, r_send, r_recv, FAR - 2, c)

    def collect(i, carry):
        k = FAR - 2 - i
        for c in range(CHUNKS):
            gather_part(k, c)
            rs_arrived(k + 1, c)
            for way in range(2):
                pass_on(way, k, c)
            if c < 2:
                exchange(obuf, ybuf, r_send, r_recv, k - 1, c)
            else:
                pl.when(k > 1)(lambda: exchange(obuf, ybuf, r_send, r_recv, k - 1, c))
        return carry

    lax.fori_loop(0, FAR - 2, collect, 0)
    for i, (src, dst) in enumerate(weights):
        remote(src, dst, w_send.at[i], w_recv.at[i], partner).wait_send()
    metas(1, NZ - 1).wait_send()
    some_totals().wait_send()
    blocks = tok.at[pl.ds(0, NZ - 1)]
    remote(blocks, blocks, ag_send, ag_recv.at[0, 0], z_peer(1)).wait_send()
    rows = sbuf.at[pl.ds(0, FAR), :, pl.ds(0, (PEERS - 1) * UNIT)]
    remote(rows, rows, d_send, d_recv.at[0, 0], x_peer(1)).wait_send()

    for c in range(2):
        gather_part(0, c)
        for q in range(2):
            rs_arrived(1, c + 2 * q)
        for q in range(2):
            chunk = c + 2 * q
            out[:, block(chunk)] = (
                part[q * TOK : (q + 1) * TOK, :] + rs_in[UP, 0, chunk].astype(F32) + rs_in[DOWN, 0, chunk].astype(F32)
            ).astype(BF)

    remote(rows, rows, r_send, r_recv.at[0, 0], x_peer(1)).wait_send()
    sums = rs_out.at[:, :, :, pl.ds(0, TOK * (NZ - 1) // NZ)]
    remote(sums, sums, rs_send, rs_recv.at[0, 0], z_peer(1)).wait_send()


def on_device(tokens, expert_ids, route_probs, shard_limit, gate_proj, up_proj, down_proj):
    dma = pltpu.SemaphoreType.DMA
    anywhere = pl.BlockSpec(memory_space=pltpu.HBM)
    near = pl.BlockSpec(memory_space=pltpu.VMEM)
    unit = (FAR + 1, CHUNKS, ROWS, COLS)
    operands = (tokens, expert_ids.T, route_probs.T, shard_limit, gate_proj, up_proj, down_proj)
    ring = (2, FAR, CHUNKS)
    return pl.pallas_call(
        kernel,
        out_shape=jax.ShapeDtypeStruct((TOK, WIDTH), BF),
        in_specs=[anywhere] * len(operands),
        out_specs=near,
        scratch_shapes=[
            pltpu.VMEM((8, TOK), jnp.int32),
            pltpu.VMEM((8, TOK), F32),
            pltpu.VMEM((1, EXPERTS), jnp.int32),
            pltpu.VMEM((NZ, CHUNKS, TOK, COLS), BF),
            pltpu.VMEM((NZ, 2 * SLOTS, EXPERTS), F32),
            pltpu.VMEM((NX, 8, EXPERTS), F32),
            pltpu.VMEM((WIDTH, HIDDEN), BF),
            pltpu.VMEM((WIDTH, HIDDEN), BF),
            pltpu.VMEM((HIDDEN, WIDTH), BF),
            pltpu.VMEM(unit, BF),
            pltpu.VMEM(unit, BF),
            pltpu.VMEM((ROWS, HIDDEN), F32),
            pltpu.VMEM((ROWS, HIDDEN), F32),
            pltpu.VMEM((ROWS, HIDDEN), BF),
            pltpu.VMEM(unit, BF),
            pltpu.VMEM(unit, BF),
            pltpu.VMEM((FAR + 1, 2 * TOK, ROWS), BF),
            pltpu.VMEM((FAR + 1, 2 * TOK, ROWS), BF),
            pltpu.VMEM((2 * TOK, COLS), F32),
            pltpu.VMEM((*ring, TOK, COLS), BF),
            pltpu.VMEM((*ring, TOK, COLS), BF),
            dma((3,)), dma, dma((3,)), dma((3,)), dma((3,)), dma, dma((FAR,)), dma, dma,
            dma, dma(ring[1:]), dma, dma(unit[:2]), dma, dma(unit[:2]), dma, dma(ring[1:]),
        ],
        compiler_params=pltpu.CompilerParams(
            collective_id=0, has_side_effects=True, vmem_limit_bytes=56000000
        ),
        name="expert_layer",
    )(*(pltpu.with_memory_space_constraint(array, pltpu.HBM) for array in operands))


def solution(mesh):
    whole = ("dp", "expert")
    in_specs = (
        P(whole, None), P(whole, None), P(whole, None), P(whole, None),
        P(whole, None, None), P(whole, None, None), P(whole, None, None),
    )
    return jax.shard_map(
        on_device, mesh=mesh, in_specs=in_specs, out_specs=P(whole, None), check_vma=False
    )
```
